256 devices in a mesh: ang: 32 (over y, z_hi, x), slab: 8 (over z_lo, core).
Axes of the slice: x: 4, y: 4, z: 8 (z_hi: 2, z_lo: 4; z = z_hi * 4 + z_lo), core: 2. Of those that a mesh axis runs over, the one named last changes fastest.
Arguments:
- updates: float32 [128, 2, 1024, 512], P('ang', None, 'slab'), may hold values from -6 to 6
- interp_tiles: bfloat16 [128, 32, 256, 128], P('ang'), may hold values from -0.25 to 0.25
- band_start: int32 [128, 32], P('ang'), may hold values from 0 to 2
- angle_id: int32 [128], P('ang'), may hold values from 0 to 127, each once
- angle_weight: float32 [128], replicated, may hold values from 0.05 to 0.5
- volume: float32 [4096, 2, 1024], P('ang', None, 'slab'), may hold values from -6 to 6
Outputs:
- volume_next: float32 [4096, 2, 1024], P('ang', None, 'slab')
- projection: float32 [128, 2, 1024, 512], P('ang', None, 'slab')
The draws below stay inside these ranges and needn't reach their ends.
Inputs may be any that keep to these rules, and one draw needn't show every extreme that they name: Tile j of angle slot a reads detector columns 128 * band_start[a, j] up to 256 further. `angle_id`: each measured angle stands in exactly one slot.
All inputs are finite; a program needn't handle non-finite values.
Results may differ from the reference program's by a relative error of at most 0.0062.
Values may be sent and summed in bfloat16 or wider, within the bound.
No kernel may reach another device: no remote copies, remote signals or barrier semaphores. Data moves between devices by JAX's collectives and lax.ppermute only.
A program may use at most 128 MiB of HBM per device.

```python
import math
import jax
import jax.numpy as jnp
from jax import lax

S = 512
BLOCK = 128
BAND = 256
XW = 8
ANGLES = 128
Z = 1024
CELLS = 4096
TILES = 32


def with_ends(entries, own_key, low, largest):
    index_at = [jax.random.randint(jax.random.fold_in(own_key, axis), (), 0, length) for axis, length in enumerate(entries.shape)]
    longest = entries.shape.index(max(entries.shape))
    beside = index_at[:longest] + [(index_at[longest] + 1) % entries.shape[longest]] + index_at[longest + 1:]
    return entries.at[tuple(index_at)].set(low).at[tuple(beside)].set(largest)


def strengthened(values, stream_key, source, target, parts, factor):
    owner, partner = [(jnp.arange(values.shape[dim]) // (values.shape[dim] // parts)).reshape([-1 if axis == dim else 1 for axis in range(values.ndim)]) for dim in (source, target)]
    chosen = jax.random.permutation(stream_key, parts)[partner]
    strong = (owner == chosen) | (owner == (partner + parts // 2) % parts)
    return jnp.where(strong, factor * values, values)


def steps_of(rng, shape, pieces, smallest, largest):
    factor_of, own = 1.0, jax.random.fold_in(rng, 6)
    for position, blocks in pieces:
        steps = jnp.exp(jax.random.uniform(jax.random.fold_in(own, position), (blocks,), jnp.float32, smallest / len(pieces), largest / len(pieces)))
        factor_of = factor_of * jnp.repeat(steps, shape[position] // blocks).reshape([-1 if axis == position else 1 for axis in range(len(shape))])
    return factor_of


def gaussian(key, extent, spread, most, pieces=(), kind=jnp.bfloat16):
    drawn = spread * jax.random.normal(key, extent, jnp.float32)
    if pieces:
        drawn = drawn * steps_of(key, extent, pieces, -0.22, 0.18)
    return jnp.clip(drawn, -most, most).astype(kind)


def noise_with(rng, extent, scale, bound, pieces, heavy, held_as=jnp.bfloat16):
    values = scale * jax.random.normal(rng, extent, jnp.float32)
    if pieces:
        values = values * steps_of(rng, extent, pieces, -0.22, 0.18)
    return jnp.clip(strengthened(values, jax.random.fold_in(rng, 3), *heavy), -bound, bound).astype(held_as)


def setup_inputs(seed: int = 0) -> dict:
    streams_of = jax.random.split(jax.random.key(seed), 7)
    updates = gaussian(streams_of[0], (ANGLES, 2, Z, S), 1.0, 6.0, ((0, 32), (2, 8)), jnp.float32)
    interp_tiles = noise_with(streams_of[1], (ANGLES, TILES, BAND, BLOCK), (BAND * XW) ** -0.5, 0.25, ((0, 32),), (0, 1, 32, 2.75))
    band_start = with_ends(jax.random.randint(streams_of[2], (ANGLES, TILES), 0, S // BLOCK - 1), jax.random.fold_in(streams_of[2], 1), 0, (S // BLOCK - 1) - 1).astype(jnp.int32)
    angle_id = jax.random.permutation(streams_of[3], ANGLES).astype(jnp.int32)
    angle_weight = jnp.clip(jnp.exp(jax.random.uniform(streams_of[4], (ANGLES,), jnp.float32, math.log(0.05), math.log(0.5))), 0.05, 0.5)
    volume = gaussian(streams_of[5], (CELLS, 2, Z), 1.0, 6.0, ((0, 32), (2, 8)), jnp.float32)
    return dict(updates=updates, interp_tiles=interp_tiles, band_start=band_start, angle_id=angle_id, angle_weight=angle_weight, volume=volume)


SMOOTHING = 0.25


def clamp_absorption(field):
    channel = jnp.arange(2, dtype=jnp.int32)[None, :, None]
    return jnp.where(channel == 1, jnp.maximum(field, 0.0), field)


def band_windows(row_block, starts):
    def take_window(first_block):
        return lax.dynamic_slice_in_dim(row_block, first_block * BLOCK, BAND, axis=1)
    return jax.vmap(take_window)(starts)


def place_bands(images, starts):
    positions = jnp.arange(S // BLOCK - 1, dtype=jnp.int32)
    onehot = (starts[:, None] == positions[None, :]).astype(jnp.float32)
    grouped = jnp.einsum('jk,jrq->krq', onehot, images, precision=lax.Precision.HIGHEST)
    result = jnp.zeros((images.shape[1], S), jnp.float32)
    for offset_index in range(S // BLOCK - 1):
        result = result + jnp.pad(grouped[offset_index], ((0, 0), (BLOCK * offset_index, S - BLOCK * offset_index - BAND)))
    return result


def reference(updates, interp_tiles, band_start, angle_id, angle_weight, volume):
    row_count = 2 * Z
    matches = angle_id[:, None] == jnp.arange(ANGLES, dtype=jnp.int32)[None, :]
    chosen = jnp.sum(jnp.where(matches, angle_weight[None, :], 0.0), axis=1)
    scaled = (chosen[:, None, None, None] * updates).astype(jnp.bfloat16).reshape(ANGLES, row_count, S)

    def back_step(summed, packed):
        row_block, tile_set, starts = packed
        windows = band_windows(row_block, starts).astype(jnp.float32)
        term = jnp.einsum('jrq,jqp->jpr', windows, tile_set.astype(jnp.float32))
        return summed + term, 0

    initial = jnp.zeros((TILES, BLOCK, row_count), jnp.float32)
    summed = lax.scan(back_step, initial, (scaled, interp_tiles, band_start))[0]
    partial_sum = summed.reshape(CELLS, 2, Z)
    padded = jnp.pad(volume, ((0, 0), (0, 0), (1, 1)))
    smooth = volume - SMOOTHING * (2.0 * volume - padded[:, :, :-2] - padded[:, :, 2:])
    volume_next = clamp_absorption(smooth + partial_sum)
    lowered = lax.optimization_barrier(volume_next.astype(jnp.bfloat16))
    lowered = lowered.astype(jnp.float32).reshape(TILES, BLOCK, row_count)

    def forward_one(packed):
        tile_set, starts = packed
        images = jnp.einsum('jpr,jqp->jrq', lowered, tile_set.astype(jnp.float32))
        return place_bands(images, starts)

    projection = lax.map(forward_one, (interp_tiles, band_start))
    return volume_next, projection.reshape(ANGLES, 2, Z, S)
```

```python
import functools

import jax
import jax.numpy as jnp
from jax import lax
from jax.experimental import pallas as pl
from jax.experimental.pallas import tpu as pltpu
from jax.sharding import PartitionSpec as P

SMOOTHING = 0.25
YS, ZS, XS = 4, 2, 4
LINE = 4
STEP = 2
FAR = (2, 1, 3)
ORDER = [(1, d) for d in FAR] + [(0, d) for d in FAR] + [(1, 0), (0, 0)]
OTHER, SAME, OWN = 0, 12, 24


def tile_table(me):
    y, zh, x = me // (ZS * XS), (me // XS) % ZS, me % XS
    other = jnp.array([o for o, _ in ORDER for _ in range(LINE)], jnp.int32)
    d = jnp.array([d for _, d in ORDER for _ in range(LINE)], jnp.int32)
    k = jnp.array([k for _ in ORDER for k in range(LINE)], jnp.int32)
    owner = jnp.where(other == 1, 1 - zh, zh)
    dy = jnp.where(owner == 0, k, d)
    dx = jnp.where(owner == 0, d, k)
    return ((y + dy) % YS) * (ZS * XS) + owner * XS + (x + dx) % XS


def moves(other, first, delta):
    pairs = []
    for y in range(YS):
        for zh in range(ZS):
            for x in range(XS):
                along_x = (zh ^ other == 0) == first
                ty, tx = (y, (x + delta) % XS) if along_x else ((y + delta) % YS, x)
                pairs.append(((y * ZS + zh) * XS + x, (ty * ZS + zh) * XS + tx))
    return pairs


def moved(value, other, first, delta):
    return lax.ppermute(value, "ang", moves(other, first, delta))


def across(value):
    half = [(a, a ^ XS) for a in range(YS * ZS * XS)]
    return lax.ppermute(value, "ang", half)


def params(mib, **more):
    return pltpu.CompilerParams(vmem_limit_bytes=mib << 20, **more)


def scale_kernel(ids, weights, updates, volume, scaled, cells, head, tail):
    a = pl.program_id(0)
    weight = weights[ids[a]]
    depth = updates.shape[2]
    for c in range(2):
        scaled[0, c * depth : (c + 1) * depth, :] = (weight * updates[0, c]).astype(jnp.bfloat16)

    @pl.when(a == 0)
    def _():
        for c in range(2):
            cells[c * depth : (c + 1) * depth, :] = volume[:, c, :].T
        for c in range(2):
            head[c : c + 1, :] = cells[c * depth : c * depth + 1, :]
            tail[c : c + 1, :] = cells[(c + 1) * depth - 1 : (c + 1) * depth, :]


def scale(updates, volume, ids, weights):
    angles, _, depth, detector = updates.shape
    share = volume.shape[0]
    rows = 2 * depth
    return pl.pallas_call(
        scale_kernel,
        grid_spec=pltpu.PrefetchScalarGridSpec(
            num_scalar_prefetch=2,
            grid=(angles,),
            in_specs=[
                pl.BlockSpec((1, 2, depth, detector), lambda a, *_: (a, 0, 0, 0)),
                pl.BlockSpec((share, 2, depth), lambda a, *_: (0, 0, 0)),
            ],
            out_specs=[
                pl.BlockSpec((1, rows, detector), lambda a, *_: (a, 0, 0)),
                pl.BlockSpec((rows, share), lambda a, *_: (0, 0)),
                pl.BlockSpec((2, share), lambda a, *_: (0, 0)),
                pl.BlockSpec((2, share), lambda a, *_: (0, 0)),
            ],
        ),
        out_shape=[
            jax.ShapeDtypeStruct((angles, rows, detector), jnp.bfloat16),
            jax.ShapeDtypeStruct((rows, share), jnp.float32),
            jax.ShapeDtypeStruct((2, share), jnp.float32),
            jax.ShapeDtypeStruct((2, share), jnp.float32),
        ],
        compiler_params=params(16),
        cost_estimate=pl.CostEstimate(flops=1 << 22, bytes_accessed=4 << 20, transcendentals=0),
        name="scale",
    )(ids, weights, updates, volume)


def back_kernel(base, groups, block, table, starts, scaled, *refs):
    tiles, outs = refs[:STEP], refs[STEP:]
    i = pl.program_id(0)
    per = LINE // STEP
    results = []
    for u in range(STEP):
        j = table[base + i * STEP + u]
        total = None
        for a in range(scaled.shape[0]):
            start = pl.multiple_of(starts[a, j] * block, block)
            window = scaled[a, :, pl.ds(start, 2 * block)]
            part = jnp.dot(window, tiles[u][a, 0], preferred_element_type=jnp.float32)
            total = part if total is None else total + part
        results.append(total)
    for g in range(groups):

        @pl.when(i // per == g)
        def _(g=g):
            for u in range(STEP):
                outs[g][u] = results[u].astype(outs[g].dtype)


def back(scaled, tiles, table, starts, base, groups, dtype):
    angles, rows, detector = scaled.shape
    _, _, band, block = tiles.shape
    per = LINE // STEP
    return pl.pallas_call(
        functools.partial(back_kernel, base, groups, block),
        grid_spec=pltpu.PrefetchScalarGridSpec(
            num_scalar_prefetch=2,
            grid=(groups * per,),
            in_specs=[pl.BlockSpec((angles, rows, detector), lambda i, *_: (0, 0, 0))]
            + [
                pl.BlockSpec(
                    (angles, 1, band, block),
                    lambda i, table, starts, u=u: (0, table[base + i * STEP + u], 0, 0),
                )
                for u in range(STEP)
            ],
            out_specs=[
                pl.BlockSpec(
                    (STEP, rows, block),
                    lambda i, *_, g=g: (jnp.clip(i - g * per, 0, per - 1), 0, 0),
                )
                for g in range(groups)
            ],
        ),
        out_shape=[jax.ShapeDtypeStruct((LINE, rows, block), dtype)] * groups,
        compiler_params=params(16),
        cost_estimate=pl.CostEstimate(
            flops=2 * groups * LINE * angles * rows * band * block,
            bytes_accessed=groups * LINE * angles * band * block * 2,
            transcendentals=0,
        ),
        name="back",
    )(table, starts, scaled, *([tiles] * STEP))


def step_kernel(cells, before, after, own, s1, s2, s3, crossed, lowered, following):
    rows, share = cells.shape
    depth = rows // 2
    z = lax.broadcasted_iota(jnp.int32, (depth, share), 0)
    for c in range(2):
        at = slice(c * depth, (c + 1) * depth)
        value = cells[at, :]
        down = jnp.where(z == 0, before[c : c + 1, :], pltpu.roll(value, 1, 0))
        up = jnp.where(z == depth - 1, after[c : c + 1, :], pltpu.roll(value, depth - 1, 0))
        smooth = value - SMOOTHING * (2.0 * value - down - up)
        added = own[at, :]
        for ref in (s1, s2, s3, crossed):
            added = added + ref[at, :].astype(jnp.float32)
        result = smooth + added
        if c == 1:
            result = jnp.maximum(result, 0.0)
        following[at, :] = result
        lowered[at, :] = result.astype(jnp.bfloat16)


def volume_step(cells, before, after, own, arrived, crossed):
    whole = pl.BlockSpec(memory_space=pltpu.VMEM)
    return pl.pallas_call(
        step_kernel,
        in_specs=[whole] * 8,
        out_specs=[whole] * 2,
        out_shape=[
            jax.ShapeDtypeStruct(cells.shape, jnp.bfloat16),
            jax.ShapeDtypeStruct(cells.shape, jnp.float32),
        ],
        compiler_params=params(8),
        cost_estimate=pl.CostEstimate(flops=1 << 20, bytes_accessed=1 << 19, transcendentals=0),
        name="volume_step",
    )(cells, before, after, own, *arrived, crossed)


def turn_kernel(following, volume):
    depth = volume.shape[2]
    for c in range(2):
        volume[:, c, :] = following[c * depth : (c + 1) * depth, :].T


def turn(following, shape):
    whole = pl.BlockSpec(memory_space=pltpu.VMEM)
    return pl.pallas_call(
        turn_kernel,
        in_specs=[whole],
        out_specs=whole,
        out_shape=jax.ShapeDtypeStruct(shape, jnp.float32),
        compiler_params=params(8),
        cost_estimate=pl.CostEstimate(flops=1 << 20, bytes_accessed=1 << 18, transcendentals=0),
        name="turn",
    )(following)


def forward_kernel(base, groups, block, chained, table, starts, *refs):
    pieces, refs = refs[:groups], refs[groups:]
    tiles, refs = refs[:STEP], refs[STEP:]
    if chained:
        held, refs = refs[0], refs[1:]
    image, piece = refs
    i = pl.program_id(0)
    per = LINE // STEP

    @pl.when(i == 0)
    def _():
        image[...] = held[...] if chained else jnp.zeros_like(image)

    for g in range(groups):

        @pl.when(i // per == g)
        def _(g=g):
            piece[...] = pieces[g][...]

    for u in range(STEP):
        j = table[base + i * STEP + u]
        for a in range(image.shape[0]):
            start = pl.multiple_of(starts[a, j] * block, block)
            part = lax.dot_general(
                piece[u],
                tiles[u][a, 0],
                (((1,), (1,)), ((), ())),
                preferred_element_type=jnp.float32,
            )
            image[a, :, pl.ds(start, 2 * block)] += part


def forward(pieces, tiles, table, starts, base, held, detector):
    groups = len(pieces)
    angles, _, band, block = tiles.shape
    rows = pieces[0].shape[1]
    per = LINE // STEP
    shape = (angles, rows, detector)
    chained = held is not None
    whole = pl.BlockSpec(shape, lambda i, *_: (0, 0, 0))
    return pl.pallas_call(
        functools.partial(forward_kernel, base, groups, block, chained),
        grid_spec=pltpu.PrefetchScalarGridSpec(
            num_scalar_prefetch=2,
            grid=(groups * per,),
            in_specs=[
                pl.BlockSpec(
                    (STEP, rows, block),
                    lambda i, *_, g=g: (jnp.clip(i - g * per, 0, per - 1), 0, 0),
                )
                for g in range(groups)
            ]
            + [
                pl.BlockSpec(
                    (angles, 1, band, block),
                    lambda i, table, starts, u=u: (0, table[base + i * STEP + u], 0, 0),
                )
                for u in range(STEP)
            ]
            + ([whole] if chained else []),
            out_specs=whole,
            scratch_shapes=[pltpu.VMEM((STEP, rows, block), jnp.bfloat16)],
        ),
        out_shape=jax.ShapeDtypeStruct(shape, jnp.float32),
        compiler_params=params(24),
        cost_estimate=pl.CostEstimate(
            flops=2 * groups * LINE * angles * rows * band * block,
            bytes_accessed=groups * LINE * angles * band * block * 2,
            transcendentals=0,
        ),
        name="forward",
    )(table, starts, *pieces, *([tiles] * STEP), *([held] if chained else []))


def shards(updates, tiles, starts, ids, weights, volume):
    angles, _, depth, detector = updates.shape
    table = tile_table(lax.axis_index("ang"))
    count = lax.axis_size("slab")
    scaled, cells, head, tail = scale(updates, volume, ids, weights)
    before = lax.ppermute(tail, "slab", [(i, i + 1) for i in range(count - 1)])
    after = lax.ppermute(head, "slab", [(i + 1, i) for i in range(count - 1)])

    far = {}
    far[1] = back(scaled, tiles, table, starts, OTHER, 3, jnp.bfloat16)
    arrived = {1: [moved(v, 1, True, d) for v, d in zip(far[1], FAR)]}
    far[0] = back(scaled, tiles, table, starts, SAME, 3, jnp.bfloat16)
    arrived[0] = [moved(v, 0, True, d) for v, d in zip(far[0], FAR)]
    own = dict(zip((1, 0), back(scaled, tiles, table, starts, OWN, 2, jnp.float32)))

    kept, reached = {}, {}
    for other in (1, 0):
        line = own[other]
        for v in arrived[other]:
            line = line + v.astype(jnp.float32)
        kept[other] = line[0]
        reached[other] = [moved(line[d].astype(jnp.bfloat16), other, False, d) for d in FAR]
    leaving = kept[1]
    for v in reached[1]:
        leaving = leaving + v.astype(jnp.float32)
    crossed = across(leaving.astype(jnp.bfloat16))
    lowered, following = volume_step(cells, before, after, kept[0], reached[0], crossed)

    visiting = across(lowered)
    lines, rest = {}, {}
    for other, mine in ((0, lowered), (1, visiting)):
        near = {d: moved(mine, other, False, LINE - d) for d in FAR}
        lines[other] = jnp.stack([mine] + [near[d] for d in range(1, LINE)])
        rest[other] = [moved(lines[other], other, True, LINE - d) for d in FAR]
    volume_next = turn(following, volume.shape)
    image = forward([lines[1], lines[0]], tiles, table, starts, OWN, None, detector)
    image = forward(rest[0], tiles, table, starts, SAME, image, detector)
    image = forward(rest[1], tiles, table, starts, OTHER, image, detector)
    return volume_next, image.reshape(angles, 2, depth, detector)


def solution(mesh):
    placed = (
        P("ang", None, "slab", None),
        P("ang", None, None, None),
        P("ang", None),
        P("ang"),
        P(),
        P("ang", None, "slab"),
    )
    return jax.shard_map(
        shards,
        mesh=mesh,
        in_specs=placed,
        out_specs=(P("ang", None, "slab"), P("ang", None, "slab", None)),
        check_vma=False,
    )
```

```python
import functools

import jax
import jax.numpy as jnp
from jax import lax
from jax.experimental import pallas as pl
from jax.experimental.pallas import tpu as pltpu
from jax.sharding import PartitionSpec as P

SMOOTHING = 0.25
YS, ZS, XS = 4, 2, 4
LINE = 4
FAR = (2, 1, 3)
ORDER = [(1, d) for d in FAR] + [(0, d) for d in FAR] + [(1, 0), (0, 0)]
OTHER, SAME, OWN = 0, 12, 24


def moves(other, first, delta):
    pairs = []
    for y in range(YS):
        for zh in range(ZS):
            for x in range(XS):
                along_x = (zh ^ other == 0) == first
                ty, tx = (y, (x + delta) % XS) if along_x else ((y + delta) % YS, x)
                pairs.append(((y * ZS + zh) * XS + x, (ty * ZS + zh) * XS + tx))
    return pairs


def moved(value, other, first, delta):
    return lax.ppermute(value, "ang", moves(other, first, delta))


def across(value):
    half = [(a, a ^ XS) for a in range(YS * ZS * XS)]
    return lax.ppermute(value, "ang", half)


def params(mib, **more):
    return pltpu.CompilerParams(vmem_limit_bytes=mib << 20, **more)


VMEM = pl.BlockSpec(memory_space=pltpu.VMEM)
SMEM = pl.BlockSpec(memory_space=pltpu.SMEM)


AHEAD = pl.CostEstimate(flops=1 << 33, bytes_accessed=1 << 20, transcendentals=0)


def call(kernel, name, in_specs, outs, flops, mib=16):
    return pl.pallas_call(
        kernel,
        in_specs=in_specs,
        out_specs=[VMEM] * len(outs),
        out_shape=[jax.ShapeDtypeStruct(shape, dtype) for shape, dtype in outs],
        compiler_params=params(mib),
        cost_estimate=pl.CostEstimate(flops=flops, bytes_accessed=1 << 20, transcendentals=0),
        name=name,
    )


def plan_kernel(table):
    me = lax.axis_index("ang")
    y, zh, x = lax.shift_right_logical(me, 3), lax.shift_right_logical(me, 2) & 1, me & 3
    for i, (other, d, k) in enumerate((o, d, k) for o, d in ORDER for k in range(LINE)):
        owner = zh ^ other
        dy = k + owner * (d - k)
        dx = d + owner * (k - d)
        table[i] = ((y + dy) & 3) * 8 + owner * 4 + ((x + dx) & 3)


def plan():
    return pl.pallas_call(
        plan_kernel,
        out_specs=SMEM,
        out_shape=jax.ShapeDtypeStruct((len(ORDER) * LINE,), jnp.int32),
        compiler_params=params(4),
        cost_estimate=AHEAD,
        name="plan",
    )()


def edges_kernel(volume, cells, head, tail):
    depth = volume.shape[2]
    for c in range(2):
        turned = volume[:, c, :].T
        cells[c * depth : (c + 1) * depth, :] = turned
        head[c : c + 1, :] = turned[:1, :]
        tail[c : c + 1, :] = turned[depth - 1 :, :]


def edges(volume):
    share, _, depth = volume.shape
    outs = [((2 * depth, share), jnp.float32)] + [((2, share), jnp.float32)] * 2
    return call(edges_kernel, "edges", [VMEM], outs, 1 << 20, 4)(volume)


def product(scaled, held, starts, j):
    angles, _, _ = scaled.shape
    block = held.shape[3]
    windows = []
    for a in range(angles):
        start = pl.multiple_of(starts[a, j] * block, block)
        windows.append(scaled[a, :, pl.ds(start, 2 * block)])
    return jnp.dot(
        jnp.concatenate(windows, axis=1),
        jnp.concatenate([held[a, j] for a in range(angles)], axis=0),
        preferred_element_type=jnp.float32,
    )


def scale_kernel(table, ids, weights, updates, scaled):
    depth = updates.shape[2]
    for a in range(updates.shape[0]):
        weight = weights[ids[a]]
        for c in range(2):
            at = slice(c * depth, (c + 1) * depth)
            scaled[a, at, :] = (weight * updates[a, c]).astype(jnp.bfloat16)


def scale(updates, table, ids, weights):
    angles, _, depth, detector = updates.shape
    outs = [((angles, 2 * depth, detector), jnp.bfloat16)]
    return call(scale_kernel, "scale", [SMEM, SMEM, SMEM, VMEM], outs, 1 << 33, 8)(
        table, ids, weights, updates
    )[0]


def back_kernel(base, table, starts, scaled, held, *outs):
    for g, out in enumerate(outs):
        for k in range(LINE):
            i = base + g * LINE + k
            out[k] = product(scaled, held, starts, table[i]).astype(out.dtype)


def back(scaled, held, table, starts, base, groups, dtype):
    _, rows, _ = scaled.shape
    angles, _, band, block = held.shape
    outs = [((LINE, rows, block), dtype)] * groups
    flops = 2 * groups * LINE * angles * rows * band * block
    kernel = functools.partial(back_kernel, base)
    return call(kernel, "back", [SMEM, SMEM, VMEM, VMEM], outs, flops)(
        table, starts, scaled, held
    )


def line_kernel(own, s1, s2, s3, kept, *sent):
    for k in range(LINE):
        total = own[k]
        for ref in (s1, s2, s3):
            total = total + ref[k].astype(jnp.float32)
        if k == 0:
            kept[...] = total
        else:
            sent[k - 1][...] = total.astype(jnp.bfloat16)


def line_sum(own, arrived):
    tile = own.shape[1:]
    outs = [(tile, jnp.float32)] + [(tile, jnp.bfloat16)] * (LINE - 1)
    kept, *sent = call(line_kernel, "line", [VMEM] * 4, outs, 1 << 20)(own, *arrived)
    return kept, sent


def tile_kernel(kept, s1, s2, s3, total):
    result = kept[...]
    for ref in (s1, s2, s3):
        result = result + ref[...].astype(jnp.float32)
    total[...] = result.astype(total.dtype)


def tile_sum(kept, arrived):
    return call(tile_kernel, "tile", [VMEM] * 4, [(kept.shape, jnp.bfloat16)], 1 << 18, 4)(
        kept, *arrived
    )[0]


def step_kernel(cells, before, after, own, s1, s2, s3, crossed, lowered, following):
    rows, share = cells.shape
    depth = rows // 2
    z = lax.broadcasted_iota(jnp.int32, (depth, share), 0)
    for c in range(2):
        at = slice(c * depth, (c + 1) * depth)
        value = cells[at, :]
        down = jnp.where(z == 0, before[c : c + 1, :], pltpu.roll(value, 1, 0))
        up = jnp.where(z == depth - 1, after[c : c + 1, :], pltpu.roll(value, depth - 1, 0))
        smooth = value - SMOOTHING * (2.0 * value - down - up)
        added = own[at, :]
        for ref in (s1, s2, s3, crossed):
            added = added + ref[at, :].astype(jnp.float32)
        result = smooth + added
        if c == 1:
            result = jnp.maximum(result, 0.0)
        following[at, :] = result
        lowered[at, :] = result.astype(jnp.bfloat16)


def volume_step(cells, before, after, own, arrived, crossed):
    outs = [(cells.shape, jnp.bfloat16), (cells.shape, jnp.float32)]
    return call(step_kernel, "volume_step", [VMEM] * 8, outs, 1 << 20, 4)(
        cells, before, after, own, *arrived, crossed
    )


def projected(image, a, piece, held, j, starts):
    block = held.shape[3]
    start = pl.multiple_of(starts[a, j] * block, block)
    part = lax.dot_general(
        piece, held[a, j], (((1,), (1,)), ((), ())), preferred_element_type=jnp.float32
    )
    image[..., pl.ds(start, 2 * block)] += part


def first_kernel(table, starts, held, following, *refs):
    pieces, (image, volume) = refs[:-2], refs[-2:]
    depth = volume.shape[2]
    for c in range(2):
        volume[:, c, :] = following[c * depth : (c + 1) * depth, :].T

    def angle(a, carry):
        image[a] = jnp.zeros(image.shape[1:], image.dtype)
        for base, piece in zip((OWN, OWN + LINE, SAME, SAME + LINE, SAME + 2 * LINE), pieces):
            for k in range(LINE):
                i = base + k
                projected(image.at[a], a, piece[k], held, table[i], starts)
        return carry

    lax.fori_loop(0, image.shape[0], angle, 0)


def first(pieces, held, table, starts, following, image, volume):
    angles, _, band, block = held.shape
    flops = 2 * len(pieces) * LINE * angles * image[1] * band * block
    specs = [SMEM, SMEM, VMEM, VMEM] + [VMEM] * len(pieces)
    outs = [(image, jnp.float32), (volume, jnp.float32)]
    return call(first_kernel, "first", specs, outs, flops, 16)(
        table, starts, held, following, *pieces
    )


def last_kernel(table, starts, held, before, p1, p2, p3, image):
    a = pl.program_id(0)
    image[...] = before[...]
    for g, piece in enumerate((p1, p2, p3)):
        for k in range(LINE):
            i = OTHER + g * LINE + k
            projected(image.at[0], a, piece[k], held, table[i], starts)


def last(pieces, held, table, starts, before):
    angles, _, band, block = held.shape
    _, rows, detector = before.shape
    angle = pl.BlockSpec((1, rows, detector), lambda a: (a, 0, 0))
    return pl.pallas_call(
        last_kernel,
        grid=(angles,),
        in_specs=[SMEM, SMEM, VMEM, angle, VMEM, VMEM, VMEM],
        out_specs=angle,
        out_shape=jax.ShapeDtypeStruct(before.shape, jnp.float32),
        compiler_params=params(16),
        cost_estimate=pl.CostEstimate(
            flops=2 * len(pieces) * LINE * angles * rows * band * block,
            bytes_accessed=1 << 20,
            transcendentals=0,
        ),
        name="last",
    )(table, starts, held, before, *pieces)


def shards(updates, tiles, starts, ids, weights, volume):
    angles, _, depth, detector = updates.shape
    table = plan()
    count = lax.axis_size("slab")
    cells, head, tail = edges(volume)
    before = lax.ppermute(tail, "slab", [(i, i + 1) for i in range(count - 1)])
    after = lax.ppermute(head, "slab", [(i + 1, i) for i in range(count - 1)])

    arrived, own, kept, reached = {}, {}, {}, {}
    scaled, held = scale(updates, table, ids, weights), tiles
    far = back(scaled, held, table, starts, OTHER, 3, jnp.bfloat16)
    arrived[1] = [moved(v, 1, True, d) for v, d in zip(far, FAR)]
    far = back(scaled, held, table, starts, SAME, 3, jnp.bfloat16)
    arrived[0] = [moved(v, 0, True, d) for v, d in zip(far, FAR)]
    own[1], own[0] = back(scaled, held, table, starts, OWN, 2, jnp.float32)
    for other in (1, 0):
        kept[other], sent = line_sum(own[other], arrived[other])
        reached[other] = [moved(sent[d - 1], other, False, d) for d in FAR]
    crossed = across(tile_sum(kept[1], reached[1]))
    lowered, following = volume_step(cells, before, after, kept[0], reached[0], crossed)

    visiting = across(lowered)
    lines, rest = {}, {}
    for other, mine in ((0, lowered), (1, visiting)):
        near = {d: moved(mine, other, False, LINE - d) for d in FAR}
        lines[other] = jnp.stack([mine] + [near[d] for d in range(1, LINE)])
        rest[other] = [moved(lines[other], other, True, LINE - d) for d in FAR]
    image = (angles, 2 * depth, detector)
    image, volume_next = first(
        [lines[1], lines[0], *rest[0]], held, table, starts, following, image, volume.shape
    )
    image = last(rest[1], held, table, starts, image)
    return volume_next, image.reshape(angles, 2, depth, detector)


def solution(mesh):
    placed = (
        P("ang", None, "slab", None),
        P("ang", None, None, None),
        P("ang", None),
        P("ang"),
        P(),
        P("ang", None, "slab"),
    )
    return jax.shard_map(
        shards,
        mesh=mesh,
        in_specs=placed,
        out_specs=(P("ang", None, "slab"), P("ang", None, "slab", None)),
        check_vma=False,
    )
```

```python
import functools

import jax
import jax.numpy as jnp
from jax import lax
from jax.experimental import pallas as pl
from jax.experimental.pallas import tpu as pltpu
from jax.sharding import PartitionSpec as P


SMOOTHING = 0.25
YS, ZS, XS = 4, 2, 4
LINE = 4
FAR = (2, 1, 3)
ORDER = [(other, d) for d in (*FAR, 0) for other in (1, 0)]


def moves(other, first, delta):
    pairs = []
    for y in range(YS):
        for zh in range(ZS):
            for x in range(XS):
                along_x = (zh ^ other == 0) == first
                ty, tx = (y, (x + delta) % XS) if along_x else ((y + delta) % YS, x)
                pairs.append(((y * ZS + zh) * XS + x, (ty * ZS + zh) * XS + tx))
    return pairs


def moved(value, other, first, delta):
    return lax.ppermute(value, "ang", moves(other, first, delta))


def place(other, d):
    return ORDER.index((other, d)) * LINE


def across(value):
    half = [(a, a ^ XS) for a in range(YS * ZS * XS)]
    return lax.ppermute(value, "ang", half)


def params(mib, **more):
    return pltpu.CompilerParams(vmem_limit_bytes=mib << 20, **more)


VMEM = pl.BlockSpec(memory_space=pltpu.VMEM)
SMEM = pl.BlockSpec(memory_space=pltpu.SMEM)


AHEAD = pl.CostEstimate(flops=1 << 33, bytes_accessed=1 << 20, transcendentals=0)


def call(kernel, in_specs, outs, flops, mib=16):
    return pl.pallas_call(
        kernel,
        in_specs=in_specs,
        out_specs=[VMEM] * len(outs),
        out_shape=[jax.ShapeDtypeStruct(shape, dtype) for shape, dtype in outs],
        compiler_params=params(mib),
        cost_estimate=pl.CostEstimate(flops=flops, bytes_accessed=1 << 20, transcendentals=0),
    )


def plan_kernel(table):
    me = lax.axis_index("ang")
    y, zh, x = lax.shift_right_logical(me, 3), lax.shift_right_logical(me, 2) & 1, me & 3
    for i, (other, d, k) in enumerate((o, d, k) for o, d in ORDER for k in range(LINE)):
        owner = zh ^ other
        dy = k + owner * (d - k)
        dx = d + owner * (k - d)
        table[i] = ((y + dy) & 3) * 8 + owner * 4 + ((x + dx) & 3)


def plan():
    return pl.pallas_call(
        plan_kernel,
        out_specs=SMEM,
        out_shape=jax.ShapeDtypeStruct((len(ORDER) * LINE,), jnp.int32),
        compiler_params=params(4),
        cost_estimate=AHEAD,
        name="plan",
    )()


def edges_kernel(table, volume, cells, head, tail):
    depth = volume.shape[2]
    for c in range(2):
        turned = volume[:, c, :].T
        cells[c * depth : (c + 1) * depth, :] = turned
        head[c : c + 1, :] = turned[:1, :]
        tail[c : c + 1, :] = turned[depth - 1 :, :]


def edges(volume, table):
    share, _, depth = volume.shape
    outs = [((2 * depth, share), jnp.float32)] + [((2, share), jnp.float32)] * 2
    return call(edges_kernel, [SMEM, VMEM], outs, 1 << 20, 4)(table, volume)


def product(scaled, held, starts, j):
    angles, _, _ = scaled.shape
    block = held.shape[3]
    windows = []
    for a in range(angles):
        start = pl.multiple_of(starts[a, j] * block, block)
        windows.append(scaled[a, :, pl.ds(start, 2 * block)])
    return jnp.dot(
        jnp.concatenate(windows, axis=1),
        jnp.concatenate([held[a, j] for a in range(angles)], axis=0),
        preferred_element_type=jnp.float32,
    )


def scale_kernel(table, ids, weights, updates, scaled):
    depth = updates.shape[2]
    for a in range(updates.shape[0]):
        weight = weights[ids[a]]
        for c in range(2):
            at = slice(c * depth, (c + 1) * depth)
            scaled[a, at, :] = (weight * updates[a, c]).astype(jnp.bfloat16)


def scale(updates, table, ids, weights):
    angles, _, depth, detector = updates.shape
    outs = [((angles, 2 * depth, detector), jnp.bfloat16)]
    return call(scale_kernel, [SMEM, SMEM, SMEM, VMEM], outs, 1 << 33, 8)(
        table, ids, weights, updates
    )[0]


def back_kernel(base, table, starts, scaled, held, after, *outs):
    for g, out in enumerate(outs):
        for k in range(LINE):
            i = base + g * LINE + k
            out[k] = product(scaled, held, starts, table[i]).astype(out.dtype)


def back(scaled, held, table, starts, d, dtype, after):
    _, rows, _ = scaled.shape
    angles, _, band, block = held.shape
    outs = [((LINE, rows, block), dtype)] * 2
    flops = 2 * len(outs) * LINE * angles * rows * band * block
    kernel = functools.partial(back_kernel, place(1, d))
    specs = [SMEM, SMEM, VMEM, VMEM, pl.BlockSpec(memory_space=pl.ANY)]
    return call(kernel, specs, outs, flops)(table, starts, scaled, held, after)


def line_kernel(own, s1, s2, s3, kept, *sent):
    for k in range(LINE):
        total = own[k]
        for ref in (s1, s2, s3):
            total = total + ref[k].astype(jnp.float32)
        if k == 0:
            kept[...] = total
        else:
            sent[k - 1][...] = total.astype(jnp.bfloat16)


def line_sum(own, arrived):
    tile = own.shape[1:]
    outs = [(tile, jnp.float32)] + [(tile, jnp.bfloat16)] * (LINE - 1)
    kept, *sent = call(line_kernel, [VMEM] * 4, outs, 1 << 20)(own, *arrived)
    return kept, sent


def smooth_kernel(cells, before, after, smooth):
    rows, share = cells.shape
    depth = rows // 2
    z = lax.broadcasted_iota(jnp.int32, (depth, share), 0)
    for c in range(2):
        at = slice(c * depth, (c + 1) * depth)
        value = cells[at, :]
        down = jnp.where(z == 0, before[c : c + 1, :], pltpu.roll(value, 1, 0))
        up = jnp.where(z == depth - 1, after[c : c + 1, :], pltpu.roll(value, depth - 1, 0))
        smooth[at, :] = value - SMOOTHING * (2.0 * value - down - up)


def smoothed(cells, before, after):
    outs = [(cells.shape, jnp.float32)]
    return call(smooth_kernel, [VMEM] * 3, outs, 1 << 20, 4)(cells, before, after)[0]


def merge_kernel(smooth, k0, a1, a2, a3, k1, b1, b2, b3, mine, theirs, message):
    total = smooth[...] + k0[...]
    for ref in (a1, a2, a3):
        total = total + ref[...].astype(jnp.float32)
    mine[...] = total
    message[0] = total.astype(message.dtype)
    total = k1[...]
    for ref in (b1, b2, b3):
        total = total + ref[...].astype(jnp.float32)
    theirs[...] = total
    message[1] = total.astype(message.dtype)


def merged(smooth, kept, reached):
    outs = [(smooth.shape, jnp.float32)] * 2 + [((2, *smooth.shape), jnp.bfloat16)]
    return call(merge_kernel, [VMEM] * 9, outs, 1 << 20, 4)(
        smooth, kept[0], *reached[0], kept[1], *reached[1]
    )


def finish_kernel(mine, theirs, crossed, following, own, visiting):
    depth = mine.shape[0] // 2
    for c in range(2):
        at = slice(c * depth, (c + 1) * depth)
        here = mine[at, :] + crossed[1, at, :].astype(jnp.float32)
        there = theirs[at, :] + crossed[0, at, :].astype(jnp.float32)
        if c == 1:
            here, there = jnp.maximum(here, 0.0), jnp.maximum(there, 0.0)
        following[at, :] = here
        own[at, :] = here.astype(own.dtype)
        visiting[at, :] = there.astype(visiting.dtype)


def finished(mine, theirs, crossed):
    outs = [(mine.shape, jnp.float32)] + [(mine.shape, jnp.bfloat16)] * 2
    return call(finish_kernel, [VMEM] * 3, outs, 1 << 20, 4)(mine, theirs, crossed)


def projected(image, a, piece, held, j, starts):
    block = held.shape[3]
    start = pl.multiple_of(starts[a, j] * block, block)
    part = lax.dot_general(
        piece, held[a, j], (((1,), (1,)), ((), ())), preferred_element_type=jnp.float32
    )
    image[..., pl.ds(start, 2 * block)] += part


def near_kernel(table, starts, held, following, p1, p0, image, volume):
    depth = volume.shape[2]
    for c in range(2):
        volume[:, c, :] = following[c * depth : (c + 1) * depth, :].T

    def angle(a, carry):
        image[a] = jnp.zeros(image.shape[1:], image.dtype)
        for base, piece in ((place(1, 0), p1), (place(0, 0), p0)):
            for k in range(LINE):
                projected(image.at[a], a, piece[k], held, table[base + k], starts)
        return carry

    lax.fori_loop(0, image.shape[0], angle, 0)


def near(pieces, held, table, starts, following, image, volume):
    angles, _, band, block = held.shape
    flops = 2 * len(pieces) * LINE * angles * image[1] * band * block
    specs = [SMEM, SMEM] + [VMEM] * 4
    outs = [(image, jnp.float32), (volume, jnp.float32)]
    return call(near_kernel, specs, outs, flops, 16)(table, starts, held, following, *pieces)


def next_kernel(table, starts, held, before, p1, p2, p3, image):
    def angle(a, carry):
        image[a] = before[a]
        for d, piece in zip(FAR, (p1, p2, p3)):
            for k in range(LINE):
                projected(image.at[a], a, piece[k], held, table[place(0, d) + k], starts)
        return carry

    lax.fori_loop(0, image.shape[0], angle, 0)


def following_image(pieces, held, table, starts, before):
    angles, _, band, block = held.shape
    flops = 2 * len(pieces) * LINE * angles * before.shape[1] * band * block
    specs = [SMEM, SMEM] + [VMEM] * 5
    return call(next_kernel, specs, [(before.shape, jnp.float32)], flops, 16)(
        table, starts, held, before, *pieces
    )[0]


def last_kernel(table, starts, held, before, p1, p2, p3, image):
    a = pl.program_id(0)
    image[...] = before[...]
    for d, piece in zip(FAR, (p1, p2, p3)):
        for k in range(LINE):
            projected(image.at[0], a, piece[k], held, table[place(1, d) + k], starts)


def last(pieces, held, table, starts, before):
    angles, _, band, block = held.shape
    _, rows, detector = before.shape
    angle = pl.BlockSpec((1, rows, detector), lambda a: (a, 0, 0))
    return pl.pallas_call(
        last_kernel,
        grid=(angles,),
        in_specs=[SMEM, SMEM, VMEM, angle, VMEM, VMEM, VMEM],
        out_specs=angle,
        out_shape=jax.ShapeDtypeStruct(before.shape, jnp.float32),
        compiler_params=params(16),
        cost_estimate=pl.CostEstimate(
            flops=2 * len(pieces) * LINE * angles * rows * band * block,
            bytes_accessed=1 << 20,
            transcendentals=0,
        ),
        name="last",
    )(table, starts, held, before, *pieces)


def steps(updates, tiles, starts, ids, weights, volume):
    angles, _, depth, detector = updates.shape
    table = plan()
    count = lax.axis_size("slab")
    cells, head, tail = edges(volume, table)
    before = lax.ppermute(tail, "slab", [(i, i + 1) for i in range(count - 1)])
    after = lax.ppermute(head, "slab", [(i + 1, i) for i in range(count - 1)])

    arrived, own, kept, reached = {0: [], 1: []}, {}, {}, {}
    scaled = scale(updates, table, ids, weights)
    previous = scaled
    for d in FAR:
        far = back(scaled, tiles, table, starts, d, jnp.bfloat16, previous)
        previous = far[0]
        for other in (1, 0):
            arrived[other].append(moved(far[1 - other], other, True, d))
    own[1], own[0] = back(scaled, tiles, table, starts, 0, jnp.float32, previous)
    for other in (1, 0):
        kept[other], sent = line_sum(own[other], arrived[other])
        reached[other] = [moved(sent[d - 1], other, False, d) for d in FAR]
    mine, theirs, message = merged(smoothed(cells, before, after), kept, reached)
    following, lowered, visiting = finished(mine, theirs, across(message))

    lines, rest = {}, {}
    for other, block in ((0, lowered), (1, visiting)):
        came = {}
        for d in FAR:
            came[d] = moved(block, other, False, LINE - d)
        lines[other] = jnp.stack([block] + [came[d] for d in range(1, LINE)])
        rest[other] = []
        for d in FAR:
            rest[other].append(moved(lines[other], other, True, LINE - d))
    image = (angles, 2 * depth, detector)
    image, volume_next = near(
        [lines[1], lines[0]], tiles, table, starts, following, image, volume.shape
    )
    image = following_image(rest[0], tiles, table, starts, image)
    image = last(rest[1], tiles, table, starts, image)
    return volume_next, image.reshape(angles, 2, depth, detector)


def solution(mesh):
    placed = (
        P("ang", None, "slab", None),
        P("ang", None, None, None),
        P("ang", None),
        P("ang"),
        P(),
        P("ang", None, "slab"),
    )
    return jax.shard_map(
        steps,
        mesh=mesh,
        in_specs=placed,
        out_specs=(P("ang", None, "slab"), P("ang", None, "slab", None)),
        check_vma=False,
    )
```

```python
import functools

import jax
import jax.numpy as jnp
from jax import lax
from jax.experimental import pallas as pl
from jax.experimental.pallas import tpu as pltpu
from jax.sharding import PartitionSpec as P


SMOOTHING = 0.25
YS, ZS, XS = 4, 2, 4
LINE = 4
FAR = (2, 1, 3)
ORDER = [(other, d) for d in (*FAR, 0) for other in (1, 0)]


def moves(other, first, delta):
    pairs = []
    for y in range(YS):
        for zh in range(ZS):
            for x in range(XS):
                along_x = (zh ^ other == 0) == first
                ty, tx = (y, (x + delta) % XS) if along_x else ((y + delta) % YS, x)
                pairs.append(((y * ZS + zh) * XS + x, (ty * ZS + zh) * XS + tx))
    return pairs


def moved(value, other, first, delta):
    return lax.ppermute(value, "ang", moves(other, first, delta))


def place(other, d):
    return ORDER.index((other, d)) * LINE


def across(value):
    half = [(a, a ^ XS) for a in range(YS * ZS * XS)]
    return lax.ppermute(value, "ang", half)


def params(mib, **more):
    return pltpu.CompilerParams(vmem_limit_bytes=mib << 20, **more)


VMEM = pl.BlockSpec(memory_space=pltpu.VMEM)
SMEM = pl.BlockSpec(memory_space=pltpu.SMEM)


AHEAD = pl.CostEstimate(flops=1 << 33, bytes_accessed=1 << 20, transcendentals=0)


def call(kernel, in_specs, outs, flops, mib=16):
    return pl.pallas_call(
        kernel,
        in_specs=in_specs,
        out_specs=[VMEM] * len(outs),
        out_shape=[jax.ShapeDtypeStruct(shape, dtype) for shape, dtype in outs],
        compiler_params=params(mib),
        cost_estimate=pl.CostEstimate(flops=flops, bytes_accessed=1 << 20, transcendentals=0),
    )


def plan_kernel(table):
    me = lax.axis_index("ang")
    y, zh, x = lax.shift_right_logical(me, 3), lax.shift_right_logical(me, 2) & 1, me & 3
    for i, (other, d, k) in enumerate((o, d, k) for o, d in ORDER for k in range(LINE)):
        owner = zh ^ other
        dy = k + owner * (d - k)
        dx = d + owner * (k - d)
        table[i] = ((y + dy) & 3) * 8 + owner * 4 + ((x + dx) & 3)


def plan():
    return pl.pallas_call(
        plan_kernel,
        out_specs=SMEM,
        out_shape=jax.ShapeDtypeStruct((len(ORDER) * LINE,), jnp.int32),
        compiler_params=params(4),
        cost_estimate=AHEAD,
        name="plan",
    )()


def edges_kernel(table, volume, cells, head, tail):
    depth = volume.shape[2]
    for c in range(2):
        turned = volume[:, c, :].T
        cells[c * depth : (c + 1) * depth, :] = turned
        head[c : c + 1, :] = turned[:1, :]
        tail[c : c + 1, :] = turned[depth - 1 :, :]


def edges(volume, table):
    share, _, depth = volume.shape
    outs = [((2 * depth, share), jnp.float32)] + [((2, share), jnp.float32)] * 2
    return call(edges_kernel, [SMEM, VMEM], outs, 1 << 20, 4)(table, volume)


def product(scaled, held, starts, j):
    angles, _, _ = scaled.shape
    block = held.shape[3]
    windows = []
    for a in range(angles):
        start = pl.multiple_of(starts[a, j] * block, block)
        windows.append(scaled[a, :, pl.ds(start, 2 * block)])
    return jnp.dot(
        jnp.concatenate(windows, axis=1),
        jnp.concatenate([held[a, j] for a in range(angles)], axis=0),
        preferred_element_type=jnp.float32,
    )


def scale_kernel(table, ids, weights, updates, scaled):
    depth = updates.shape[2]
    for a in range(updates.shape[0]):
        weight = weights[ids[a]]
        for c in range(2):
            at = slice(c * depth, (c + 1) * depth)
            scaled[a, at, :] = (weight * updates[a, c]).astype(jnp.bfloat16)


def scale(updates, table, ids, weights):
    angles, _, depth, detector = updates.shape
    outs = [((angles, 2 * depth, detector), jnp.bfloat16)]
    return call(scale_kernel, [SMEM, SMEM, SMEM, VMEM], outs, 1 << 33, 8)(
        table, ids, weights, updates
    )[0]


def back_kernel(base, table, starts, scaled, held, after, *outs):
    for g, out in enumerate(outs):
        for k in range(LINE):
            i = base + g * LINE + k
            out[k] = product(scaled, held, starts, table[i]).astype(out.dtype)


def back(scaled, held, table, starts, d, dtype, after):
    _, rows, _ = scaled.shape
    angles, _, band, block = held.shape
    outs = [((LINE, rows, block), dtype)] * 2
    flops = 2 * len(outs) * LINE * angles * rows * band * block
    kernel = functools.partial(back_kernel, place(1, d))
    specs = [SMEM, SMEM, VMEM, VMEM, pl.BlockSpec(memory_space=pl.ANY)]
    return call(kernel, specs, outs, flops)(table, starts, scaled, held, after)


def line_kernel(own, s1, s2, s3, kept, *sent):
    for k in range(LINE):
        total = own[k]
        for ref in (s1, s2, s3):
            total = total + ref[k].astype(jnp.float32)
        if k == 0:
            kept[...] = total
        else:
            sent[k - 1][...] = total.astype(jnp.bfloat16)


def line_sum(own, arrived):
    tile = own.shape[1:]
    outs = [(tile, jnp.float32)] + [(tile, jnp.bfloat16)] * (LINE - 1)
    kept, *sent = call(line_kernel, [VMEM] * 4, outs, 1 << 20)(own, *arrived)
    return kept, sent


def smooth_kernel(cells, before, after, smooth):
    rows, share = cells.shape
    depth = rows // 2
    z = lax.broadcasted_iota(jnp.int32, (depth, share), 0)
    for c in range(2):
        at = slice(c * depth, (c + 1) * depth)
        value = cells[at, :]
        down = jnp.where(z == 0, before[c : c + 1, :], pltpu.roll(value, 1, 0))
        up = jnp.where(z == depth - 1, after[c : c + 1, :], pltpu.roll(value, depth - 1, 0))
        smooth[at, :] = value - SMOOTHING * (2.0 * value - down - up)


def smoothed(cells, before, after):
    outs = [(cells.shape, jnp.float32)]
    return call(smooth_kernel, [VMEM] * 3, outs, 1 << 20, 4)(cells, before, after)[0]


def merge_kernel(smooth, k0, a1, a2, a3, k1, b1, b2, b3, mine, theirs, message):
    total = smooth[...] + k0[...]
    for ref in (a1, a2, a3):
        total = total + ref[...].astype(jnp.float32)
    mine[...] = total
    message[0] = total.astype(message.dtype)
    total = k1[...]
    for ref in (b1, b2, b3):
        total = total + ref[...].astype(jnp.float32)
    theirs[...] = total
    message[1] = total.astype(message.dtype)


def merged(smooth, kept, reached):
    outs = [(smooth.shape, jnp.float32)] * 2 + [((2, *smooth.shape), jnp.bfloat16)]
    return call(merge_kernel, [VMEM] * 9, outs, 1 << 20, 4)(
        smooth, kept[0], *reached[0], kept[1], *reached[1]
    )


def finish_kernel(mine, theirs, crossed, following, own, visiting):
    depth = mine.shape[0] // 2
    for c in range(2):
        at = slice(c * depth, (c + 1) * depth)
        here = mine[at, :] + crossed[1, at, :].astype(jnp.float32)
        there = theirs[at, :] + crossed[0, at, :].astype(jnp.float32)
        if c == 1:
            here, there = jnp.maximum(here, 0.0), jnp.maximum(there, 0.0)
        following[at, :] = here
        own[at, :] = here.astype(own.dtype)
        visiting[at, :] = there.astype(visiting.dtype)


def finished(mine, theirs, crossed):
    outs = [(mine.shape, jnp.float32)] + [(mine.shape, jnp.bfloat16)] * 2
    return call(finish_kernel, [VMEM] * 3, outs, 1 << 20, 4)(mine, theirs, crossed)


NEAR = ((1, 0), (0, 0))
NEXT = tuple((0, d) for d in FAR)
LAST = tuple((1, d) for d in FAR)


def spread_kernel(table, starts, tiles, after, *outs):
    block = tiles.shape[3]
    zeros = jnp.zeros((block, block), tiles.dtype)

    def angle(a, carry):
        for out, groups in zip(outs, (NEAR, NEXT, LAST)):
            for g, (other, d) in enumerate(groups):
                for k in range(LINE):
                    j = table[place(other, d) + k]
                    first = starts[a, j]
                    column = slice((g * LINE + k) * block, (g * LINE + k + 1) * block)
                    for empty in (jnp.where(first == 0, 2, 0), jnp.where(first == 2, 1, 3)):
                        at = pl.ds(pl.multiple_of(empty * block, block), block)
                        out[a, at, column] = zeros
                    at = pl.ds(pl.multiple_of(first * block, block), 2 * block)
                    out[a, at, column] = tiles[a, j]
        return carry

    lax.fori_loop(0, tiles.shape[0], angle, 0)


def spread(tiles, table, starts, detector, after):
    angles, _, _, block = tiles.shape
    outs = [
        ((angles, detector, len(groups) * LINE * block), tiles.dtype)
        for groups in (NEAR, NEXT, LAST)
    ]
    specs = [SMEM, SMEM, VMEM, pl.BlockSpec(memory_space=pl.ANY)]
    return call(spread_kernel, specs, outs, 1 << 31, 16)(table, starts, tiles, after)


def projected(pieces, weights):
    row = jnp.concatenate([piece[k] for piece in pieces for k in range(LINE)], axis=1)
    return lax.dot_general(
        row, weights, (((1,), (1,)), ((), ())), preferred_element_type=jnp.float32
    )


def near_kernel(weights, following, p1, p0, image, volume):
    depth = volume.shape[2]
    for c in range(2):
        volume[:, c, :] = following[c * depth : (c + 1) * depth, :].T
    for a in range(image.shape[0]):
        image[a] = projected((p1, p0), weights[a])


def near(pieces, weights, following, image, volume):
    outs = [(image, jnp.float32), (volume, jnp.float32)]
    flops = 2 * weights.size * image[1]
    return call(near_kernel, [VMEM] * 4, outs, flops, 16)(weights, following, *pieces)


def next_kernel(weights, before, p1, p2, p3, image):
    for a in range(image.shape[0]):
        image[a] = before[a] + projected((p1, p2, p3), weights[a])


def further(pieces, weights, before):
    outs = [(before.shape, jnp.float32)]
    flops = 2 * weights.size * before.shape[1]
    return call(next_kernel, [VMEM] * 5, outs, flops, 16)(weights, before, *pieces)[0]


def last_kernel(weights, before, p1, p2, p3, image):
    a = pl.program_id(0)
    image[0] = before[a] + projected((p1, p2, p3), weights[a])


def last(pieces, weights, before):
    angles, rows, detector = before.shape
    return pl.pallas_call(
        last_kernel,
        grid=(angles,),
        in_specs=[VMEM] * 5,
        out_specs=pl.BlockSpec((1, rows, detector), lambda a: (a, 0, 0)),
        out_shape=jax.ShapeDtypeStruct(before.shape, jnp.float32),
        compiler_params=params(16),
        cost_estimate=pl.CostEstimate(
            flops=2 * weights.size * rows, bytes_accessed=1 << 20, transcendentals=0
        ),
        name="last",
    )(weights, before, *pieces)


def steps(updates, tiles, starts, ids, weights, volume):
    angles, _, depth, detector = updates.shape
    table = plan()
    count = lax.axis_size("slab")
    cells, head, tail = edges(volume, table)
    before = lax.ppermute(tail, "slab", [(i, i + 1) for i in range(count - 1)])
    after = lax.ppermute(head, "slab", [(i + 1, i) for i in range(count - 1)])

    arrived, own, kept, reached = {0: [], 1: []}, {}, {}, {}
    scaled = scale(updates, table, ids, weights)
    previous = scaled
    for d in FAR:
        far = back(scaled, tiles, table, starts, d, jnp.bfloat16, previous)
        previous = far[0]
        for other in (1, 0):
            arrived[other].append(moved(far[1 - other], other, True, d))
    own[1], own[0] = back(scaled, tiles, table, starts, 0, jnp.float32, previous)
    for other in (1, 0):
        kept[other], sent = line_sum(own[other], arrived[other])
        reached[other] = [moved(sent[d - 1], other, False, d) for d in FAR]
    mine, theirs, message = merged(smoothed(cells, before, after), kept, reached)
    crossed = across(message)
    weights = spread(tiles, table, starts, detector, message)
    following, lowered, visiting = finished(mine, theirs, crossed)

    lines, rest = {}, {}
    for other, block in ((0, lowered), (1, visiting)):
        came = {}
        for d in FAR:
            came[d] = moved(block, other, False, LINE - d)
        lines[other] = jnp.stack([block] + [came[d] for d in range(1, LINE)])
        rest[other] = []
        for d in FAR:
            rest[other].append(moved(lines[other], other, True, LINE - d))
    image = (angles, 2 * depth, detector)
    image, volume_next = near([lines[1], lines[0]], weights[0], following, image, volume.shape)
    image = further(rest[0], weights[1], image)
    image = last(rest[1], weights[2], image)
    return volume_next, image.reshape(angles, 2, depth, detector)


def solution(mesh):
    placed = (
        P("ang", None, "slab", None),
        P("ang", None, None, None),
        P("ang", None),
        P("ang"),
        P(),
        P("ang", None, "slab"),
    )
    return jax.shard_map(
        steps,
        mesh=mesh,
        in_specs=placed,
        out_specs=(P("ang", None, "slab"), P("ang", None, "slab", None)),
        check_vma=False,
    )
```

```python
import functools

import jax
import jax.numpy as jnp
from jax import lax
from jax.experimental import pallas as pl
from jax.experimental.pallas import tpu as pltpu
from jax.sharding import PartitionSpec as P


SMOOTHING = 0.25
YS, ZS, XS, SLABS = 4, 2, 4, 8
LINE = 4
FAR = (2, 1, 3)
ORDER = (*FAR, 0)


def position():
    me, core = lax.axis_index("ang"), lax.axis_index("slab") & 1
    y, zh, x = lax.shift_right_logical(me, 3), lax.shift_right_logical(me, 2) & 1, me & 3
    return y, zh, x, 1 - core


def moved(value, first, delta):
    pairs = []
    for y in range(YS):
        for zh in range(ZS):
            for x in range(XS):
                for slab in range(SLABS):
                    along_x = (slab % 2 == 1) == first
                    ty, tx = (y, (x + delta) % XS) if along_x else ((y + delta) % YS, x)
                    source, target = (y * ZS + zh) * XS + x, (ty * ZS + zh) * XS + tx
                    pairs.append((source * SLABS + slab, target * SLABS + slab))
    return lax.ppermute(value, ("ang", "slab"), pairs)


def across(value):
    return lax.ppermute(value, "ang", [(a, a ^ XS) for a in range(YS * ZS * XS)])


def swapped(value):
    return lax.ppermute(value, "slab", [(i, i ^ 1) for i in range(SLABS)])


def place(d):
    return ORDER.index(d) * LINE


def params(mib, **more):
    return pltpu.CompilerParams(vmem_limit_bytes=mib << 20, **more)


VMEM = pl.BlockSpec(memory_space=pltpu.VMEM)
SMEM = pl.BlockSpec(memory_space=pltpu.SMEM)
ANY = pl.BlockSpec(memory_space=pl.ANY)
AHEAD = pl.CostEstimate(flops=1 << 33, bytes_accessed=1 << 20, transcendentals=0)


def call(kernel, in_specs, outs, flops, mib=16):
    return pl.pallas_call(
        kernel,
        in_specs=in_specs,
        out_specs=[VMEM] * len(outs),
        out_shape=[jax.ShapeDtypeStruct(shape, dtype) for shape, dtype in outs],
        compiler_params=params(mib),
        cost_estimate=pl.CostEstimate(flops=flops, bytes_accessed=1 << 20, transcendentals=0),
    )


def plan_kernel(table):
    y, _, x, owner = position()
    for i, (d, k) in enumerate((d, k) for d in ORDER for k in range(LINE)):
        dy = k + owner * (d - k)
        dx = d + owner * (k - d)
        table[i] = ((y + dy) & 3) * 8 + owner * 4 + ((x + dx) & 3)


def plan():
    return pl.pallas_call(
        plan_kernel,
        out_specs=SMEM,
        out_shape=jax.ShapeDtypeStruct((len(ORDER) * LINE,), jnp.int32),
        compiler_params=params(4),
        cost_estimate=AHEAD,
        name="plan",
    )()


def edges_kernel(volume, after, cells, head, tail):
    depth = volume.shape[2]
    for c in range(2):
        turned = volume[:, c, :].T
        cells[c * depth : (c + 1) * depth, :] = turned
        head[c : c + 1, :] = turned[:1, :]
        tail[c : c + 1, :] = turned[depth - 1 :, :]


def edges(volume, after):
    share, _, depth = volume.shape
    outs = [((2 * depth, share), jnp.float32)] + [((2, share), jnp.float32)] * 2
    return call(edges_kernel, [VMEM, ANY], outs, 1 << 20, 4)(volume, after)


def scale_kernel(table, ids, weights, updates, scaled):
    depth = updates.shape[2]
    for a in range(updates.shape[0]):
        weight = weights[ids[a]]
        for c in range(2):
            at = slice(c * depth, (c + 1) * depth)
            scaled[a, at, :] = (weight * updates[a, c]).astype(jnp.bfloat16)


def scale(updates, table, ids, weights):
    angles, _, depth, detector = updates.shape
    outs = [((angles, 2 * depth, detector), jnp.bfloat16)]
    return call(scale_kernel, [SMEM, SMEM, SMEM, VMEM], outs, 1 << 33, 8)(
        table, ids, weights, updates
    )[0]


def product(sources, tiles, starts, j):
    angles, _, _, block = tiles.shape
    rows = []
    for source in sources:
        windows = []
        for a in range(angles):
            start = pl.multiple_of(starts[a, j] * block, block)
            windows.append(source[a, :, pl.ds(start, 2 * block)])
        rows.append(jnp.concatenate(windows, axis=1))
    weights = jnp.concatenate([tiles[a, j] for a in range(angles)], axis=0)
    return jnp.dot(
        jnp.concatenate(rows, axis=0), weights, preferred_element_type=jnp.float32
    )


def own_kernel(ds, table, starts, scaled, tiles, *outs):
    for d, out in zip(ds, outs):
        for k in range(LINE):
            j = table[place(d) + k]
            out[k] = product((scaled,), tiles, starts, j).astype(out.dtype)


def own_rows(scaled, tiles, table, starts, ds):
    angles, _, band, block = tiles.shape
    rows = scaled.shape[1]
    outs = [((LINE, rows, block), jnp.bfloat16)] * len(ds)
    flops = 2 * len(ds) * LINE * angles * rows * band * block
    kernel = functools.partial(own_kernel, ds)
    return call(kernel, [SMEM, SMEM, VMEM, VMEM], outs, flops)(
        table, starts, scaled, tiles
    )


def join_kernel(d, table, starts, other, tiles, own, after, out):
    rows = other.shape[1]
    for k in range(LINE):
        j = table[place(d) + k]
        out[k, :rows, :] = own[k]
        out[k, rows:, :] = product((other,), tiles, starts, j).astype(out.dtype)


def joined(other, tiles, table, starts, d, own, after):
    angles, _, band, block = tiles.shape
    rows = other.shape[1]
    outs = [((LINE, 2 * rows, block), jnp.bfloat16)]
    flops = 2 * LINE * angles * rows * band * block
    kernel = functools.partial(join_kernel, d)
    specs = [SMEM, SMEM, VMEM, VMEM, VMEM, ANY]
    return call(kernel, specs, outs, flops)(table, starts, other, tiles, own, after)[0]


def both_kernel(d, table, starts, scaled, other, tiles, after, out):
    for k in range(LINE):
        j = table[place(d) + k]
        out[k] = product((scaled, other), tiles, starts, j).astype(out.dtype)


def both_rows(scaled, other, tiles, table, starts, d, dtype, after):
    angles, _, band, block = tiles.shape
    rows = 2 * scaled.shape[1]
    flops = 2 * LINE * angles * rows * band * block
    kernel = functools.partial(both_kernel, d)
    specs = [SMEM, SMEM, VMEM, VMEM, VMEM, ANY]
    return call(kernel, specs, [((LINE, rows, block), dtype)], flops)(
        table, starts, scaled, other, tiles, after
    )[0]


def line_kernel(own, s1, s2, s3, after, kept, *sent):
    for k in range(LINE):
        total = own[k]
        for ref in (s1, s2, s3):
            total = total + ref[k].astype(jnp.float32)
        if k == 0:
            kept[...] = total
        else:
            sent[k - 1][...] = total.astype(jnp.bfloat16)


def line_sum(own, arrived, after):
    tile = own.shape[1:]
    outs = [(tile, jnp.float32)] + [(tile, jnp.bfloat16)] * (LINE - 1)
    kept, *sent = call(line_kernel, [VMEM] * 4 + [ANY], outs, 1 << 20)(
        own, *arrived, after
    )
    return kept, sent


def smooth_kernel(cells, before, after, smooth):
    rows, share = cells.shape
    depth = rows // 2
    z = lax.broadcasted_iota(jnp.int32, (depth, share), 0)
    for c in range(2):
        at = slice(c * depth, (c + 1) * depth)
        value = cells[at, :]
        down = jnp.where(z == 0, before[c : c + 1, :], pltpu.roll(value, 1, 0))
        up = jnp.where(z == depth - 1, after[c : c + 1, :], pltpu.roll(value, depth - 1, 0))
        smooth[at, :] = value - SMOOTHING * (2.0 * value - down - up)


def smoothed(cells, before, after):
    outs = [(cells.shape, jnp.float32)]
    return call(smooth_kernel, [VMEM] * 3, outs, 1 << 20, 4)(cells, before, after)[0]


def merge_kernel(smooth, beside, kept, s1, s2, s3, mine, message):
    _, zh, _, owner = position()
    rows = smooth.shape[0]
    for at, part in ((slice(0, rows), smooth), (slice(rows, 2 * rows), beside)):
        total = kept[at, :]
        for ref in (s1, s2, s3):
            total = total + ref[at, :].astype(jnp.float32)
        total = jnp.where(zh == owner, total + part[...], total)
        mine[at, :] = total
        message[at, :] = total.astype(message.dtype)


def merged(smooth, beside, kept, reached):
    outs = [(kept.shape, jnp.float32), (kept.shape, jnp.bfloat16)]
    return call(merge_kernel, [VMEM] * 6, outs, 1 << 20, 4)(
        smooth, beside, kept, *reached
    )


def finish_kernel(mine, crossed, own, beside, lowered):
    rows, _ = own.shape
    depth = rows // 2
    for slab, out in enumerate((own, beside)):
        for c in range(2):
            at = slice(slab * rows + c * depth, slab * rows + (c + 1) * depth)
            value = mine[at, :] + crossed[at, :].astype(jnp.float32)
            if c == 1:
                value = jnp.maximum(value, 0.0)
            out[c * depth : (c + 1) * depth, :] = value
            lowered[at, :] = value.astype(lowered.dtype)


def finished(mine, crossed):
    rows, share = mine.shape
    outs = [((rows // 2, share), jnp.float32)] * 2 + [(mine.shape, jnp.bfloat16)]
    return call(finish_kernel, [VMEM] * 2, outs, 1 << 20, 4)(mine, crossed)


def turn_kernel(own, received, volume):
    _, zh, _, owner = position()
    depth = volume.shape[2]
    for c in range(2):
        at = slice(c * depth, (c + 1) * depth)
        volume[:, c, :] = jnp.where(zh == owner, own[at, :], received[at, :]).T


def turned(own, received, shape):
    return call(turn_kernel, [VMEM] * 2, [(shape, jnp.float32)], 1 << 20, 4)(own, received)[0]


PARTS = ((0,), (2, 1), (3,))


def spread_kernel(table, starts, tiles, after, *outs):
    block = tiles.shape[3]
    zeros = jnp.zeros((block, block), tiles.dtype)

    def angle(a, carry):
        for out, ds in zip(outs, PARTS):
            for g, d in enumerate(ds):
                for k in range(LINE):
                    j = table[place(d) + k]
                    first = starts[a, j]
                    column = slice((g * LINE + k) * block, (g * LINE + k + 1) * block)
                    for empty in (jnp.where(first == 0, 2, 0), jnp.where(first == 2, 1, 3)):
                        at = pl.ds(pl.multiple_of(empty * block, block), block)
                        out[a, at, column] = zeros
                    at = pl.ds(pl.multiple_of(first * block, block), 2 * block)
                    out[a, at, column] = tiles[a, j]
        return carry

    lax.fori_loop(0, tiles.shape[0], angle, 0)


def spread(tiles, table, starts, detector, after):
    angles, _, _, block = tiles.shape
    outs = [((angles, detector, len(ds) * LINE * block), tiles.dtype) for ds in PARTS]
    return call(spread_kernel, [SMEM, SMEM, VMEM, ANY], outs, 1 << 31, 16)(
        table, starts, tiles, after
    )


def projected(pieces, weights):
    row = jnp.concatenate([piece[k] for piece in pieces for k in range(LINE)], axis=1)
    return lax.dot_general(
        row, weights, (((1,), (1,)), ((), ())), preferred_element_type=jnp.float32
    )


def near_kernel(weights, piece, image):
    for a in range(image.shape[0]):
        image[a] = projected((piece,), weights[a])


def near(piece, weights):
    angles, detector, _ = weights.shape
    rows = piece.shape[1]
    outs = [((angles, rows, detector), jnp.float32)]
    flops = 2 * weights.size * rows
    return call(near_kernel, [VMEM] * 2, outs, flops, 16)(weights, piece)[0]


def next_kernel(weights, before, p1, p2, image):
    for a in range(image.shape[0]):
        image[a] = before[a] + projected((p1, p2), weights[a])


def further(pieces, weights, before):
    outs = [(before.shape, jnp.float32)]
    flops = 2 * weights.size * before.shape[1]
    return call(next_kernel, [VMEM] * 4, outs, flops, 16)(weights, before, *pieces)[0]


def last_kernel(base, weights, before, piece, after, own, message):
    rows = own.shape[1]
    for i in range(own.shape[0]):
        value = before[base + i] + projected((piece,), weights[base + i])
        own[i] = value[:rows]
        message[i] = value[rows:].astype(message.dtype)


def last(piece, weights, before, base, count, after):
    _, rows, detector = before.shape
    shape = (count, rows // 2, detector)
    outs = [(shape, jnp.float32), (shape, jnp.bfloat16)]
    flops = weights.size * rows
    kernel = functools.partial(last_kernel, base)
    return call(kernel, [VMEM] * 3 + [ANY], outs, flops, 16)(
        weights, before, piece, after
    )


def leave_kernel(own0, own1, got0, got1, out, image, done):
    half = own0.shape[0]
    copies = []
    for h, (own, got) in enumerate(((own0, got0), (own1, got1))):
        for i in range(half):
            a = h * half + i
            image[a] = own[i] + got[i].astype(jnp.float32)
            copies.append(pltpu.make_async_copy(image.at[a], out.at[a], done.at[a]))
            copies[-1].start()
    for copy in copies:
        copy.wait()


def leave(own, got):
    half, rows, detector = own[0].shape
    shape = (2 * half, rows, detector)
    return pl.pallas_call(
        leave_kernel,
        in_specs=[VMEM] * 4,
        out_specs=ANY,
        out_shape=jax.ShapeDtypeStruct(shape, jnp.float32),
        scratch_shapes=[pltpu.VMEM(shape, jnp.float32), pltpu.SemaphoreType.DMA((2 * half,))],
        compiler_params=params(16),
        cost_estimate=pl.CostEstimate(flops=1 << 20, bytes_accessed=1 << 20, transcendentals=0),
        name="leave",
    )(*own, *got)


def steps(updates, tiles, starts, ids, weights, volume):
    angles, _, depth, detector = updates.shape
    count = lax.axis_size("slab")
    table = plan()
    scaled = scale(updates, table, ids, weights)
    other = swapped(scaled)
    own2, own1 = own_rows(scaled, tiles, table, starts, (2, 1))
    sent = {}
    sent[2] = joined(other, tiles, table, starts, 2, own2, own1)
    sent[1] = joined(other, tiles, table, starts, 1, own1, sent[2])
    sent[3] = both_rows(scaled, other, tiles, table, starts, 3, jnp.bfloat16, sent[1])
    own = both_rows(scaled, other, tiles, table, starts, 0, jnp.float32, sent[3])
    arrived = []
    for d in FAR:
        arrived.append(moved(sent[d], True, d))

    cells, head, tail = edges(volume, own)
    before = lax.ppermute(tail, "slab", [(i, i + 1) for i in range(count - 1)])
    after = lax.ppermute(head, "slab", [(i + 1, i) for i in range(count - 1)])
    kept, sent = line_sum(own, arrived, cells)
    reached = [moved(sent[d - 1], False, d) for d in FAR]
    smooth = smoothed(cells, before, after)
    mine, message = merged(smooth, swapped(smooth), kept, reached)
    crossed = across(message)
    bands = spread(tiles, table, starts, detector, message)
    own, beside, lowered = finished(mine, crossed)

    came = {}
    for d in FAR:
        came[d] = moved(lowered, False, LINE - d)
    beside, came[1], came[2], came[3] = lax.optimization_barrier(
        (beside, came[1], came[2], came[3])
    )
    line = jnp.stack([lowered] + [came[d] for d in range(1, LINE)])
    rest = {}
    for d in FAR:
        rest[d] = moved(line, True, LINE - d)
    received = swapped(beside)
    volume_next = turned(own, received, volume.shape)
    image = near(line, bands[0])
    image = further([rest[2], rest[1]], bands[1], image)
    half = angles // 2
    own0, message0 = last(rest[3], bands[2], image, 0, half, image)
    got0 = swapped(message0)
    own1, message1 = last(rest[3], bands[2], image, half, half, message0)
    got1 = swapped(message1)
    projection = leave([own0, own1], [got0, got1])
    return volume_next, projection.reshape(angles, 2, depth, detector)


def solution(mesh):
    placed = (
        P("ang", None, "slab", None),
        P("ang", None, None, None),
        P("ang", None),
        P("ang"),
        P(),
        P("ang", None, "slab"),
    )
    return jax.shard_map(
        steps,
        mesh=mesh,
        in_specs=placed,
        out_specs=(P("ang", None, "slab"), P("ang", None, "slab", None)),
        check_vma=False,
    )
```

```python
import functools

import jax
import jax.numpy as jnp
from jax import lax
from jax.experimental import pallas as pl
from jax.experimental.pallas import tpu as pltpu
from jax.sharding import PartitionSpec as P


SMOOTHING = 0.25
YS, ZS, XS, SLABS = 4, 2, 4, 8
LINE = 4
FAR = (2, 1, 3)
ORDER = (*FAR, 0)


def position():
    me, core = lax.axis_index("ang"), lax.axis_index("slab") & 1
    y, zh, x = lax.shift_right_logical(me, 3), lax.shift_right_logical(me, 2) & 1, me & 3
    return y, zh, x, 1 - core


def moved(value, first, delta):
    pairs = []
    for y in range(YS):
        for zh in range(ZS):
            for x in range(XS):
                for slab in range(SLABS):
                    along_x = (slab % 2 == 1) == first
                    ty, tx = (y, (x + delta) % XS) if along_x else ((y + delta) % YS, x)
                    source, target = (y * ZS + zh) * XS + x, (ty * ZS + zh) * XS + tx
                    pairs.append((source * SLABS + slab, target * SLABS + slab))
    return lax.ppermute(value, ("ang", "slab"), pairs)


def across(value):
    return lax.ppermute(value, "ang", [(a, a ^ XS) for a in range(YS * ZS * XS)])


def swapped(value):
    return lax.ppermute(value, "slab", [(i, i ^ 1) for i in range(SLABS)])


def place(d):
    return ORDER.index(d) * LINE


def params(mib, **more):
    return pltpu.CompilerParams(vmem_limit_bytes=mib << 20, **more)


VMEM = pl.BlockSpec(memory_space=pltpu.VMEM)
SMEM = pl.BlockSpec(memory_space=pltpu.SMEM)
ANY = pl.BlockSpec(memory_space=pl.ANY)
AHEAD = pl.CostEstimate(flops=1 << 33, bytes_accessed=1 << 20, transcendentals=0)


def call(kernel, in_specs, outs, flops, mib=16):
    return pl.pallas_call(
        kernel,
        in_specs=in_specs,
        out_specs=[VMEM] * len(outs),
        out_shape=[jax.ShapeDtypeStruct(shape, dtype) for shape, dtype in outs],
        compiler_params=params(mib),
        cost_estimate=pl.CostEstimate(flops=flops, bytes_accessed=1 << 20, transcendentals=0),
    )


def plan_kernel(table):
    y, _, x, owner = position()
    for i, (d, k) in enumerate((d, k) for d in ORDER for k in range(LINE)):
        dy = k + owner * (d - k)
        dx = d + owner * (k - d)
        table[i] = ((y + dy) & 3) * 8 + owner * 4 + ((x + dx) & 3)


def plan():
    return pl.pallas_call(
        plan_kernel,
        out_specs=SMEM,
        out_shape=jax.ShapeDtypeStruct((len(ORDER) * LINE,), jnp.int32),
        compiler_params=params(4),
        cost_estimate=AHEAD,
        name="plan",
    )()


def edges_kernel(volume, after, cells, inner, outer):
    depth = volume.shape[2]
    core = lax.axis_index("slab") & 1
    for c in range(2):
        turned = volume[:, c, :].T
        cells[c * depth : (c + 1) * depth, :] = turned
        head, tail = turned[:1, :], turned[depth - 1 :, :]
        inner[c : c + 1, :] = jnp.where(core == 0, tail, head)
        outer[c : c + 1, :] = jnp.where(core == 0, head, tail)


def edges(volume, after):
    share, _, depth = volume.shape
    outs = [((2 * depth, share), jnp.float32)] + [((2, share), jnp.float32)] * 2
    return call(edges_kernel, [VMEM, ANY], outs, 1 << 20, 4)(volume, after)


def scale_kernel(table, ids, weights, updates, scaled):
    depth = updates.shape[2]
    for a in range(updates.shape[0]):
        weight = weights[ids[a]]
        for c in range(2):
            at = slice(c * depth, (c + 1) * depth)
            scaled[a, at, :] = (weight * updates[a, c]).astype(jnp.bfloat16)


def scale(updates, table, ids, weights):
    angles, _, depth, detector = updates.shape
    outs = [((angles, 2 * depth, detector), jnp.bfloat16)]
    return call(scale_kernel, [SMEM, SMEM, SMEM, VMEM], outs, 1 << 33, 8)(
        table, ids, weights, updates
    )[0]


def product(sources, tiles, starts, j):
    angles, _, _, block = tiles.shape
    rows = []
    for source in sources:
        windows = []
        for a in range(angles):
            start = pl.multiple_of(starts[a, j] * block, block)
            windows.append(source[a, :, pl.ds(start, 2 * block)])
        rows.append(jnp.concatenate(windows, axis=1))
    weights = jnp.concatenate([tiles[a, j] for a in range(angles)], axis=0)
    return jnp.dot(
        jnp.concatenate(rows, axis=0), weights, preferred_element_type=jnp.float32
    )


def own_kernel(ds, table, starts, scaled, tiles, *outs):
    for d, out in zip(ds, outs):
        for k in range(LINE):
            j = table[place(d) + k]
            out[k] = product((scaled,), tiles, starts, j).astype(out.dtype)


def own_rows(scaled, tiles, table, starts, ds):
    angles, _, band, block = tiles.shape
    rows = scaled.shape[1]
    outs = [((LINE, rows, block), jnp.bfloat16)] * len(ds)
    flops = 2 * len(ds) * LINE * angles * rows * band * block
    kernel = functools.partial(own_kernel, ds)
    return call(kernel, [SMEM, SMEM, VMEM, VMEM], outs, flops)(
        table, starts, scaled, tiles
    )


def join_kernel(d, table, starts, other, tiles, own, after, first, rest):
    rows = other.shape[1]
    for k in range(LINE):
        j = table[place(d) + k]
        out = first if k == 0 else rest.at[k - 1]
        out[:rows, :] = own[k]
        out[rows:, :] = product((other,), tiles, starts, j).astype(out.dtype)


def joined(other, tiles, table, starts, d, own, after):
    angles, _, band, block = tiles.shape
    rows = other.shape[1]
    outs = [((2 * rows, block), jnp.bfloat16), ((LINE - 1, 2 * rows, block), jnp.bfloat16)]
    flops = 2 * LINE * angles * rows * band * block
    kernel = functools.partial(join_kernel, d)
    specs = [SMEM, SMEM, VMEM, VMEM, VMEM, ANY]
    return call(kernel, specs, outs, flops)(table, starts, other, tiles, own, after)


def both_kernel(d, table, starts, scaled, other, tiles, after, first, rest):
    for k in range(LINE):
        j = table[place(d) + k]
        out = first if k == 0 else rest.at[k - 1]
        out[...] = product((scaled, other), tiles, starts, j).astype(out.dtype)


def both_rows(scaled, other, tiles, table, starts, d, dtype, after):
    angles, _, band, block = tiles.shape
    rows = 2 * scaled.shape[1]
    flops = 2 * LINE * angles * rows * band * block
    kernel = functools.partial(both_kernel, d)
    specs = [SMEM, SMEM, VMEM, VMEM, VMEM, ANY]
    outs = [((rows, block), dtype), ((LINE - 1, rows, block), dtype)]
    return call(kernel, specs, outs, flops)(table, starts, scaled, other, tiles, after)


def line_kernel(own, s1, s2, s3, *sent):
    for k in range(LINE - 1):
        total = own[k]
        for ref in (s1, s2, s3):
            total = total + ref[k].astype(jnp.float32)
        sent[k][...] = total.astype(jnp.bfloat16)


def line_sum(own, arrived):
    outs = [(own.shape[1:], jnp.bfloat16)] * (LINE - 1)
    return call(line_kernel, [VMEM] * 4, outs, 1 << 20)(own, *arrived)


def smooth_kernel(cells, inner, outer, smooth):
    rows, share = cells.shape
    depth = rows // 2
    core = lax.axis_index("slab") & 1
    before = jnp.where(core == 0, outer[...], inner[...])
    after = jnp.where(core == 0, inner[...], outer[...])
    z = lax.broadcasted_iota(jnp.int32, (depth, share), 0)
    for c in range(2):
        at = slice(c * depth, (c + 1) * depth)
        value = cells[at, :]
        down = jnp.where(z == 0, before[c : c + 1, :], pltpu.roll(value, 1, 0))
        up = jnp.where(z == depth - 1, after[c : c + 1, :], pltpu.roll(value, depth - 1, 0))
        smooth[at, :] = value - SMOOTHING * (2.0 * value - down - up)


def smoothed(cells, inner, outer):
    outs = [(cells.shape, jnp.float32)]
    return call(smooth_kernel, [VMEM] * 3, outs, 1 << 20, 4)(cells, inner, outer)[0]


def merge_kernel(smooth, beside, own, a1, a2, a3, s1, s2, s3, mine, message):
    _, zh, _, owner = position()
    rows = smooth.shape[0]
    for at, part in ((slice(0, rows), smooth), (slice(rows, 2 * rows), beside)):
        total = own[at, :]
        for ref in (a1, a2, a3, s1, s2, s3):
            total = total + ref[at, :].astype(jnp.float32)
        total = jnp.where(zh == owner, total + part[...], total)
        mine[at, :] = total
        message[at, :] = total.astype(message.dtype)


def merged(smooth, beside, own, first, reached):
    outs = [(own.shape, jnp.float32), (own.shape, jnp.bfloat16)]
    return call(merge_kernel, [VMEM] * 9, outs, 1 << 20, 4)(smooth, beside, own, *first, *reached)


def finish_kernel(mine, crossed, own, beside, lowered):
    rows, _ = own.shape
    depth = rows // 2
    for slab, out in enumerate((own, beside)):
        for c in range(2):
            at = slice(slab * rows + c * depth, slab * rows + (c + 1) * depth)
            value = mine[at, :] + crossed[at, :].astype(jnp.float32)
            if c == 1:
                value = jnp.maximum(value, 0.0)
            out[c * depth : (c + 1) * depth, :] = value
            lowered[at, :] = value.astype(lowered.dtype)


def finished(mine, crossed):
    rows, share = mine.shape
    outs = [((rows // 2, share), jnp.float32)] * 2 + [(mine.shape, jnp.bfloat16)]
    return call(finish_kernel, [VMEM] * 2, outs, 1 << 20, 4)(mine, crossed)


def turn_kernel(own, received, volume, token):
    token[...] = jnp.zeros_like(token)
    _, zh, _, owner = position()
    depth = volume.shape[2]
    for c in range(2):
        at = slice(c * depth, (c + 1) * depth)
        volume[:, c, :] = jnp.where(zh == owner, own[at, :], received[at, :]).T


def turned(own, received, shape):
    outs = [(shape, jnp.float32), ((8, 128), jnp.float32)]
    return call(turn_kernel, [VMEM] * 2, outs, 1 << 20, 4)(own, received)


PARTS = ((0,), (2, 1), (3,))


def spread_kernel(table, starts, tiles, after, *outs):
    block = tiles.shape[3]
    zeros = jnp.zeros((block, block), tiles.dtype)

    def angle(a, carry):
        for out, ds in zip(outs, PARTS):
            for g, d in enumerate(ds):
                for k in range(LINE):
                    j = table[place(d) + k]
                    first = starts[a, j]
                    column = slice((g * LINE + k) * block, (g * LINE + k + 1) * block)
                    for empty in (jnp.where(first == 0, 2, 0), jnp.where(first == 2, 1, 3)):
                        at = pl.ds(pl.multiple_of(empty * block, block), block)
                        out[a, at, column] = zeros
                    at = pl.ds(pl.multiple_of(first * block, block), 2 * block)
                    out[a, at, column] = tiles[a, j]
        return carry

    lax.fori_loop(0, tiles.shape[0], angle, 0)


def spread(tiles, table, starts, detector, after):
    angles, _, _, block = tiles.shape
    outs = [((angles, detector, len(ds) * LINE * block), tiles.dtype) for ds in PARTS]
    return call(spread_kernel, [SMEM, SMEM, VMEM, ANY], outs, 1 << 31, 16)(
        table, starts, tiles, after
    )


def row_of(pieces):
    blocks = []
    for first, rest in pieces:
        blocks += [first[...]] + [rest[k] for k in range(LINE - 1)]
    return jnp.concatenate(blocks, axis=1)


def projected(pieces, weights):
    return lax.dot_general(
        row_of(pieces), weights, (((1,), (1,)), ((), ())), preferred_element_type=jnp.float32
    )


def near_kernel(weights, first, rest, image):
    for a in range(image.shape[0]):
        image[a] = projected(((first, rest),), weights[a])


def near(piece, weights):
    angles, detector, _ = weights.shape
    rows = piece[0].shape[0]
    outs = [((angles, rows, detector), jnp.float32)]
    flops = 2 * weights.size * rows
    return call(near_kernel, [VMEM] * 3, outs, flops, 16)(weights, *piece)[0]


def next_kernel(weights, before, f1, r1, f2, r2, after, image):
    for a in range(image.shape[0]):
        image[a] = before[a] + projected(((f1, r1), (f2, r2)), weights[a])


def further(pieces, weights, before, after):
    outs = [(before.shape, jnp.float32)]
    flops = 2 * weights.size * before.shape[1]
    return call(next_kernel, [VMEM] * 6 + [ANY], outs, flops, 16)(
        weights, before, *pieces[0], *pieces[1], after
    )[0]


def last_kernel(base, weights, before, first, rest, after, own, message):
    rows = own.shape[1]
    for i in range(own.shape[0]):
        value = before[base + i] + projected(((first, rest),), weights[base + i])
        own[i] = value[:rows]
        message[i] = value[rows:].astype(message.dtype)


def last(piece, weights, before, base, count, after):
    _, rows, detector = before.shape
    shape = (count, rows // 2, detector)
    outs = [(shape, jnp.float32), (shape, jnp.bfloat16)]
    flops = weights.size * rows
    kernel = functools.partial(last_kernel, base)
    return call(kernel, [VMEM] * 4 + [ANY], outs, flops, 16)(
        weights, before, *piece, after
    )


def leave_kernel(base, own, got, *refs):
    out, image, done = refs[-3:]
    copies = []
    for i in range(own.shape[0]):
        image[i] = own[i] + got[i].astype(jnp.float32)
        copies.append(pltpu.make_async_copy(image.at[i], out.at[base + i], done.at[i]))
        copies[-1].start()
    for copy in copies:
        copy.wait()


def leave(own, got, base, shape, held=None):
    half = own.shape[0]
    return pl.pallas_call(
        functools.partial(leave_kernel, base),
        in_specs=[VMEM] * 2 + [ANY] * (held is not None),
        out_specs=ANY,
        out_shape=jax.ShapeDtypeStruct(shape, jnp.float32),
        scratch_shapes=[pltpu.VMEM(own.shape, jnp.float32), pltpu.SemaphoreType.DMA((half,))],
        input_output_aliases={} if held is None else {2: 0},
        compiler_params=params(16),
        cost_estimate=pl.CostEstimate(flops=1 << 20, bytes_accessed=1 << 20, transcendentals=0),
        name="leave",
    )(own, got, *([] if held is None else [held]))


def steps(updates, tiles, starts, ids, weights, volume):
    angles, _, depth, detector = updates.shape
    count = lax.axis_size("slab")
    table = plan()
    scaled = scale(updates, table, ids, weights)
    other = swapped(scaled)
    cells, inner, outer = edges(volume, scaled)
    inner = swapped(inner)
    odd = range(1, count - 1, 2)
    outer = lax.ppermute(outer, "slab", [p for i in odd for p in ((i, i + 1), (i + 1, i))])
    own2, own1 = own_rows(scaled, tiles, table, starts, (2, 1))
    sent = {}
    sent[2] = joined(other, tiles, table, starts, 2, own2, own1)
    sent[1] = joined(other, tiles, table, starts, 1, own1, sent[2][0])
    sent[3] = both_rows(scaled, other, tiles, table, starts, 3, jnp.bfloat16, sent[1][0])
    own = both_rows(scaled, other, tiles, table, starts, 0, jnp.float32, sent[3][0])
    first, arrived = [], []
    for d in FAR:
        arrived.append(moved(sent[d][1], True, d))
    for d in FAR:
        first.append(moved(sent[d][0], True, d))
    passed = line_sum(own[1], arrived)
    reached = []
    for d in FAR:
        reached.append(moved(passed[d - 1], False, d))
    smooth = smoothed(cells, inner, outer)
    beside = swapped(smooth)
    mine, message = merged(smooth, beside, own[0], first, reached)
    crossed = across(message)
    bands = spread(tiles, table, starts, detector, message)
    own, beside, lowered = finished(mine, crossed)

    came, first = {}, {}
    for d in FAR:
        came[d] = moved(lowered, False, LINE - d)
    for d in FAR:
        first[d] = moved(lowered, True, LINE - d)
    beside, came[1], came[2], came[3] = lax.optimization_barrier(
        (beside, came[1], came[2], came[3])
    )
    line = jnp.stack([came[d] for d in range(1, LINE)])
    rest = {}
    for d in FAR:
        rest[d] = moved(line, True, LINE - d)
    received = swapped(beside)
    volume_next, token = turned(own, received, volume.shape)
    image = near((lowered, line), bands[0])
    image = further(
        [(first[2], rest[2]), (first[1], rest[1])], bands[1], image, token
    )
    half = angles // 2
    piece = first[3], rest[3]
    own0, message0 = last(piece, bands[2], image, 0, half, image)
    got0 = swapped(message0)
    own1, message1 = last(piece, bands[2], image, half, half, message0)
    got1 = swapped(message1)
    shape = (angles, 2 * depth, detector)
    projection = leave(own0, got0, 0, shape)
    projection = leave(own1, got1, half, shape, projection)
    return volume_next, projection.reshape(angles, 2, depth, detector)


def solution(mesh):
    placed = (
        P("ang", None, "slab", None),
        P("ang", None, None, None),
        P("ang", None),
        P("ang"),
        P(),
        P("ang", None, "slab"),
    )
    return jax.shard_map(
        steps,
        mesh=mesh,
        in_specs=placed,
        out_specs=(P("ang", None, "slab"), P("ang", None, "slab", None)),
        check_vma=False,
    )
```

```python
import functools

import jax
import jax.numpy as jnp
from jax import lax
from jax.experimental import pallas as pl
from jax.experimental.pallas import tpu as pltpu
from jax.sharding import PartitionSpec as P


SMOOTHING = 0.25
YS, ZS, XS, SLABS = 4, 2, 4, 8
LINE = 4
FAR = (2, 1, 3)
ORDER = (*FAR, 0)


def position():
    me, core = lax.axis_index("ang"), lax.axis_index("slab") & 1
    y, zh, x = lax.shift_right_logical(me, 3), lax.shift_right_logical(me, 2) & 1, me & 3
    return y, zh, x, 1 - core


def moved(value, first, delta):
    pairs = []
    for y in range(YS):
        for zh in range(ZS):
            for x in range(XS):
                for slab in range(SLABS):
                    along_x = (slab % 2 == 1) == first
                    ty, tx = (y, (x + delta) % XS) if along_x else ((y + delta) % YS, x)
                    source, target = (y * ZS + zh) * XS + x, (ty * ZS + zh) * XS + tx
                    pairs.append((source * SLABS + slab, target * SLABS + slab))
    return lax.ppermute(value, ("ang", "slab"), pairs)


def across(value):
    return lax.ppermute(value, "ang", [(a, a ^ XS) for a in range(YS * ZS * XS)])


def swapped(value):
    return lax.ppermute(value, "slab", [(i, i ^ 1) for i in range(SLABS)])


def place(d):
    return ORDER.index(d) * LINE


def params(mib, **more):
    return pltpu.CompilerParams(vmem_limit_bytes=mib << 20, **more)


VMEM = pl.BlockSpec(memory_space=pltpu.VMEM)
SMEM = pl.BlockSpec(memory_space=pltpu.SMEM)
ANY = pl.BlockSpec(memory_space=pl.ANY)
AHEAD = pl.CostEstimate(flops=1 << 33, bytes_accessed=1 << 20, transcendentals=0)


def call(kernel, in_specs, outs, flops, mib=16):
    return pl.pallas_call(
        kernel,
        in_specs=in_specs,
        out_specs=[VMEM] * len(outs),
        out_shape=[jax.ShapeDtypeStruct(shape, dtype) for shape, dtype in outs],
        compiler_params=params(mib),
        cost_estimate=pl.CostEstimate(flops=flops, bytes_accessed=1 << 20, transcendentals=0),
    )


def plan_kernel(table):
    y, _, x, own = position()
    for half, owner in enumerate((own, 1 - own)):
        for i, (d, k) in enumerate((d, k) for d in ORDER for k in range(LINE)):
            dy = k + owner * (d - k)
            dx = d + owner * (k - d)
            at = half * len(ORDER) * LINE + i
            table[at] = ((y + dy) & 3) * 8 + owner * 4 + ((x + dx) & 3)


def plan():
    return pl.pallas_call(
        plan_kernel,
        out_specs=SMEM,
        out_shape=jax.ShapeDtypeStruct((2 * len(ORDER) * LINE,), jnp.int32),
        compiler_params=params(4),
        cost_estimate=AHEAD,
        name="plan",
    )()


def edges_kernel(volume, after, cells, inner, outer):
    depth = volume.shape[2]
    core = lax.axis_index("slab") & 1
    for c in range(2):
        turned = volume[:, c, :].T
        cells[c * depth : (c + 1) * depth, :] = turned
        head, tail = turned[:1, :], turned[depth - 1 :, :]
        inner[c : c + 1, :] = jnp.where(core == 0, tail, head)
        outer[c : c + 1, :] = jnp.where(core == 0, head, tail)


def edges(volume, after):
    share, _, depth = volume.shape
    outs = [((2 * depth, share), jnp.float32)] + [((2, share), jnp.float32)] * 2
    return call(edges_kernel, [VMEM, ANY], outs, 1 << 20, 4)(volume, after)


def scale_kernel(table, ids, weights, updates, scaled):
    depth = updates.shape[2]
    for a in range(updates.shape[0]):
        weight = weights[ids[a]]
        for c in range(2):
            at = slice(c * depth, (c + 1) * depth)
            scaled[a, at, :] = (weight * updates[a, c]).astype(jnp.bfloat16)


def scale(updates, table, ids, weights):
    angles, _, depth, detector = updates.shape
    outs = [((angles, 2 * depth, detector), jnp.bfloat16)]
    return call(scale_kernel, [SMEM, SMEM, SMEM, VMEM], outs, 1 << 33, 8)(
        table, ids, weights, updates
    )[0]


def product(sources, tiles, starts, j):
    angles, _, _, block = tiles.shape
    rows = []
    for source in sources:
        windows = []
        for a in range(angles):
            start = pl.multiple_of(starts[a, j] * block, block)
            windows.append(source[a, :, pl.ds(start, 2 * block)])
        rows.append(jnp.concatenate(windows, axis=1))
    weights = jnp.concatenate([tiles[a, j] for a in range(angles)], axis=0)
    return jnp.dot(
        jnp.concatenate(rows, axis=0), weights, preferred_element_type=jnp.float32
    )


def own_kernel(ds, table, starts, scaled, tiles, *outs):
    for d, out in zip(ds, outs):
        for k in range(LINE):
            j = table[place(d) + k]
            out[k] = product((scaled,), tiles, starts, j).astype(out.dtype)


def own_rows(scaled, tiles, table, starts, ds):
    angles, _, band, block = tiles.shape
    rows = scaled.shape[1]
    outs = [((LINE, rows, block), jnp.bfloat16)] * len(ds)
    flops = 2 * len(ds) * LINE * angles * rows * band * block
    kernel = functools.partial(own_kernel, ds)
    return call(kernel, [SMEM, SMEM, VMEM, VMEM], outs, flops)(
        table, starts, scaled, tiles
    )


def join_kernel(d, table, starts, other, tiles, own, after, first, rest):
    rows = other.shape[1]
    for k in range(LINE):
        j = table[place(d) + k]
        out = first if k == 0 else rest.at[k - 1]
        out[:rows, :] = own[k]
        out[rows:, :] = product((other,), tiles, starts, j).astype(out.dtype)


def joined(other, tiles, table, starts, d, own, after):
    angles, _, band, block = tiles.shape
    rows = other.shape[1]
    outs = [((2 * rows, block), jnp.bfloat16), ((LINE - 1, 2 * rows, block), jnp.bfloat16)]
    flops = 2 * LINE * angles * rows * band * block
    kernel = functools.partial(join_kernel, d)
    specs = [SMEM, SMEM, VMEM, VMEM, VMEM, ANY]
    return call(kernel, specs, outs, flops)(table, starts, other, tiles, own, after)


def both_kernel(d, table, starts, scaled, other, tiles, after, first, rest):
    for k in range(LINE):
        j = table[place(d) + k]
        out = first if k == 0 else rest.at[k - 1]
        out[...] = product((scaled, other), tiles, starts, j).astype(out.dtype)


def both_rows(scaled, other, tiles, table, starts, d, dtype, after):
    angles, _, band, block = tiles.shape
    rows = 2 * scaled.shape[1]
    flops = 2 * LINE * angles * rows * band * block
    kernel = functools.partial(both_kernel, d)
    specs = [SMEM, SMEM, VMEM, VMEM, VMEM, ANY]
    outs = [((rows, block), dtype), ((LINE - 1, rows, block), dtype)]
    return call(kernel, specs, outs, flops)(table, starts, scaled, other, tiles, after)


def line_kernel(own, s1, s2, s3, *sent):
    for k in range(LINE - 1):
        total = own[k]
        for ref in (s1, s2, s3):
            total = total + ref[k].astype(jnp.float32)
        sent[k][...] = total.astype(jnp.bfloat16)


def line_sum(own, arrived):
    outs = [(own.shape[1:], jnp.bfloat16)] * (LINE - 1)
    return call(line_kernel, [VMEM] * 4, outs, 1 << 20)(own, *arrived)


def smooth_kernel(cells, inner, outer, smooth):
    rows, share = cells.shape
    depth = rows // 2
    core = lax.axis_index("slab") & 1
    before = jnp.where(core == 0, outer[...], inner[...])
    after = jnp.where(core == 0, inner[...], outer[...])
    z = lax.broadcasted_iota(jnp.int32, (depth, share), 0)
    for c in range(2):
        at = slice(c * depth, (c + 1) * depth)
        value = cells[at, :]
        down = jnp.where(z == 0, before[c : c + 1, :], pltpu.roll(value, 1, 0))
        up = jnp.where(z == depth - 1, after[c : c + 1, :], pltpu.roll(value, depth - 1, 0))
        smooth[at, :] = value - SMOOTHING * (2.0 * value - down - up)


def smoothed(cells, inner, outer):
    outs = [(cells.shape, jnp.float32)]
    return call(smooth_kernel, [VMEM] * 3, outs, 1 << 20, 4)(cells, inner, outer)[0]


def merge_kernel(smooth, beside, own, a1, a2, a3, s1, s2, s3, mine, message):
    _, zh, _, owner = position()
    rows = smooth.shape[0]
    for at, part in ((slice(0, rows), smooth), (slice(rows, 2 * rows), beside)):
        total = own[at, :]
        for ref in (a1, a2, a3, s1, s2, s3):
            total = total + ref[at, :].astype(jnp.float32)
        total = jnp.where(zh == owner, total + part[...], total)
        mine[at, :] = total
        message[at, :] = total.astype(message.dtype)


def merged(smooth, beside, own, first, reached):
    outs = [(own.shape, jnp.float32), (own.shape, jnp.bfloat16)]
    return call(merge_kernel, [VMEM] * 9, outs, 1 << 20, 4)(smooth, beside, own, *first, *reached)


def finish_kernel(mine, crossed, own, beside, lowered):
    rows, _ = own.shape
    depth = rows // 2
    for slab, out in enumerate((own, beside)):
        for c in range(2):
            at = slice(slab * rows + c * depth, slab * rows + (c + 1) * depth)
            value = mine[at, :] + crossed[at, :].astype(jnp.float32)
            if c == 1:
                value = jnp.maximum(value, 0.0)
            out[c * depth : (c + 1) * depth, :] = value
            lowered[at, :] = value.astype(lowered.dtype)


def finished(mine, crossed):
    rows, share = mine.shape
    outs = [((rows // 2, share), jnp.float32)] * 2 + [(mine.shape, jnp.bfloat16)]
    return call(finish_kernel, [VMEM] * 2, outs, 1 << 20, 4)(mine, crossed)


def turn_kernel(own, received, volume, token):
    token[...] = jnp.zeros_like(token)
    _, zh, _, owner = position()
    depth = volume.shape[2]
    for c in range(2):
        at = slice(c * depth, (c + 1) * depth)
        volume[:, c, :] = jnp.where(zh == owner, own[at, :], received[at, :]).T


def turned(own, received, shape):
    outs = [(shape, jnp.float32), ((8, 128), jnp.float32)]
    return call(turn_kernel, [VMEM] * 2, outs, 1 << 20, 4)(own, received)


GROUPS = (0, *FAR)


def spread_kernel(table, starts, tiles, after, *outs):
    block = tiles.shape[3]
    zeros = jnp.zeros((block, block), tiles.dtype)

    def angle(a, carry):
        for out, d in zip(outs, GROUPS):
            for i in range(2 * LINE):
                half, k = divmod(i, LINE)
                j = table[half * len(ORDER) * LINE + place(d) + k]
                first = starts[a, j]
                column = slice(i * block, (i + 1) * block)
                for empty in (jnp.where(first == 0, 2, 0), jnp.where(first == 2, 1, 3)):
                    at = pl.ds(pl.multiple_of(empty * block, block), block)
                    out[a, at, column] = zeros
                at = pl.ds(pl.multiple_of(first * block, block), 2 * block)
                out[a, at, column] = tiles[a, j]
        return carry

    lax.fori_loop(0, tiles.shape[0], angle, 0)


def spread(tiles, table, starts, detector, after):
    angles, _, _, block = tiles.shape
    outs = [((angles, detector, 2 * LINE * block), tiles.dtype)] * len(GROUPS)
    return call(spread_kernel, [SMEM, SMEM, VMEM, ANY], outs, 1 << 31, 16)(
        table, starts, tiles, after
    )


def cut_kernel(first, rest, out):
    rows = out.shape[1]
    out[0] = first[rows:, :]
    for k in range(1, LINE):
        out[k] = rest[k - 1, rows:, :]


def cut(first, rest):
    rows, block = first.shape
    outs = [((LINE, rows // 2, block), first.dtype)]
    return call(cut_kernel, [VMEM] * 2, outs, 1 << 18, 4)(first, rest)[0]


def own_blocks(first, rest):
    rows = first.shape[0] // 2
    return [first[:rows, :]] + [rest[k, :rows, :] for k in range(LINE - 1)]


def projected(blocks, weights):
    row = jnp.concatenate(blocks, axis=1)
    return lax.dot_general(
        row, weights, (((1,), (1,)), ((), ())), preferred_element_type=jnp.float32
    )


def image_kernel(chained, whole, weights, first, rest, *refs):
    *refs, after, image = refs
    blocks = own_blocks(first, rest)
    if whole:
        blocks += [refs[0][k] for k in range(LINE)]
    depth = sum(block.shape[1] for block in blocks)
    for a in range(image.shape[0]):
        value = projected(blocks, weights[a, :, :depth])
        image[a] = refs[-1][a] + value if chained else value


def imaged(weights, piece, got, before, after):
    angles, detector, _ = weights.shape
    rows = piece[0].shape[0] // 2
    more = [v for v in (got, before) if v is not None]
    outs = [((angles, rows, detector), jnp.float32)]
    flops = weights.size * rows * (1 if got is None else 2)
    kernel = functools.partial(image_kernel, before is not None, got is not None)
    specs = [VMEM] * (3 + len(more)) + [ANY]
    return call(kernel, specs, outs, flops)(weights, *piece, *more, after)[0]


def leave_kernel(weights, got, before, out, image, done):
    blocks = [got[k] for k in range(LINE)]
    depth = sum(block.shape[1] for block in blocks)
    copies = []
    for a in range(image.shape[0]):
        image[a] = before[a] + projected(blocks, weights[a, :, depth:])
        copies.append(pltpu.make_async_copy(image.at[a], out.at[a], done.at[a]))
        copies[-1].start()
    for copy in copies:
        copy.wait()


def leave(weights, got, before):
    shape = before.shape
    return pl.pallas_call(
        leave_kernel,
        in_specs=[VMEM] * 3,
        out_specs=ANY,
        out_shape=jax.ShapeDtypeStruct(shape, jnp.float32),
        scratch_shapes=[pltpu.VMEM(shape, jnp.float32), pltpu.SemaphoreType.DMA((shape[0],))],
        compiler_params=params(16),
        cost_estimate=pl.CostEstimate(flops=1 << 28, bytes_accessed=1 << 20, transcendentals=0),
        name="leave",
    )(weights, got, before)


def steps(updates, tiles, starts, ids, weights, volume):
    angles, _, depth, detector = updates.shape
    count = lax.axis_size("slab")
    table = plan()
    scaled = scale(updates, table, ids, weights)
    other = swapped(scaled)
    cells, inner, outer = edges(volume, scaled)
    inner = swapped(inner)
    odd = range(1, count - 1, 2)
    outer = lax.ppermute(outer, "slab", [p for i in odd for p in ((i, i + 1), (i + 1, i))])
    own2, own1 = own_rows(scaled, tiles, table, starts, (2, 1))
    sent = {}
    sent[2] = joined(other, tiles, table, starts, 2, own2, own1)
    sent[1] = joined(other, tiles, table, starts, 1, own1, sent[2][0])
    sent[3] = both_rows(scaled, other, tiles, table, starts, 3, jnp.bfloat16, sent[1][0])
    own = both_rows(scaled, other, tiles, table, starts, 0, jnp.float32, sent[3][0])
    first, arrived = [], []
    for d in FAR:
        arrived.append(moved(sent[d][1], True, d))
    for d in FAR:
        first.append(moved(sent[d][0], True, d))
    passed = line_sum(own[1], arrived)
    reached = []
    for d in FAR:
        reached.append(moved(passed[d - 1], False, d))
    smooth = smoothed(cells, inner, outer)
    beside = swapped(smooth)
    mine, message = merged(smooth, beside, own[0], first, reached)
    crossed = across(message)
    bands = dict(zip(GROUPS, spread(tiles, table, starts, detector, message)))
    own, beside, lowered = finished(mine, crossed)

    came, first = {}, {}
    for d in FAR:
        came[d] = moved(lowered, False, LINE - d)
    for d in FAR:
        first[d] = moved(lowered, True, LINE - d)
    beside, came[1], came[2], came[3] = lax.optimization_barrier(
        (beside, came[1], came[2], came[3])
    )
    line = jnp.stack([came[d] for d in range(1, LINE)])
    rest = {}
    for d in FAR:
        rest[d] = moved(line, True, LINE - d)
    received = swapped(beside)
    volume_next, token = turned(own, received, volume.shape)
    first[0], rest[0] = lowered, line
    image, last = None, token
    for d in GROUPS:
        piece = first[d], rest[d]
        got = swapped(cut(*piece))
        image = imaged(bands[d], piece, None if d == FAR[-1] else got, image, last)
        last = image
    projection = leave(bands[FAR[-1]], got, image)
    return volume_next, projection.reshape(angles, 2, depth, detector)


def solution(mesh):
    placed = (
        P("ang", None, "slab", None),
        P("ang", None, None, None),
        P("ang", None),
        P("ang"),
        P(),
        P("ang", None, "slab"),
    )
    return jax.shard_map(
        steps,
        mesh=mesh,
        in_specs=placed,
        out_specs=(P("ang", None, "slab"), P("ang", None, "slab", None)),
        check_vma=False,
    )
```

```python
import functools

import jax
import jax.numpy as jnp
from jax import lax
from jax.experimental import pallas as pl
from jax.experimental.pallas import tpu as pltpu
from jax.sharding import PartitionSpec as P


SMOOTHING = 0.25
YS, ZS, XS, SLABS = 4, 2, 4, 8
LINE = 4
FAR = (2, 1, 3)
ORDER = (*FAR, 0)


def position():
    me, core = lax.axis_index("ang"), lax.axis_index("slab") & 1
    y, zh, x = lax.shift_right_logical(me, 3), lax.shift_right_logical(me, 2) & 1, me & 3
    return y, zh, x, 1 - core


def moved(value, first, delta):
    pairs = []
    for y in range(YS):
        for zh in range(ZS):
            for x in range(XS):
                for slab in range(SLABS):
                    along_x = (slab % 2 == 1) == first
                    ty, tx = (y, (x + delta) % XS) if along_x else ((y + delta) % YS, x)
                    source, target = (y * ZS + zh) * XS + x, (ty * ZS + zh) * XS + tx
                    pairs.append((source * SLABS + slab, target * SLABS + slab))
    return lax.ppermute(value, ("ang", "slab"), pairs)


def across(value):
    return lax.ppermute(value, "ang", [(a, a ^ XS) for a in range(YS * ZS * XS)])


def swapped(value):
    return lax.ppermute(value, "slab", [(i, i ^ 1) for i in range(SLABS)])


def place(d):
    return ORDER.index(d) * LINE


def params(mib, **more):
    return pltpu.CompilerParams(vmem_limit_bytes=mib << 20, **more)


VMEM = pl.BlockSpec(memory_space=pltpu.VMEM)
SMEM = pl.BlockSpec(memory_space=pltpu.SMEM)
ANY = pl.BlockSpec(memory_space=pl.ANY)
AHEAD = pl.CostEstimate(flops=1 << 33, bytes_accessed=1 << 20, transcendentals=0)


def call(kernel, in_specs, outs, flops, mib=16):
    return pl.pallas_call(
        kernel,
        in_specs=in_specs,
        out_specs=[VMEM] * len(outs),
        out_shape=[jax.ShapeDtypeStruct(shape, dtype) for shape, dtype in outs],
        compiler_params=params(mib),
        cost_estimate=pl.CostEstimate(flops=flops, bytes_accessed=1 << 20, transcendentals=0),
    )


def plan_kernel(table):
    y, _, x, own = position()
    for half, owner in enumerate((own, 1 - own)):
        for i, (d, k) in enumerate((d, k) for d in ORDER for k in range(LINE)):
            dy = k + owner * (d - k)
            dx = d + owner * (k - d)
            at = half * len(ORDER) * LINE + i
            table[at] = ((y + dy) & 3) * 8 + owner * 4 + ((x + dx) & 3)


def plan():
    return pl.pallas_call(
        plan_kernel,
        out_specs=SMEM,
        out_shape=jax.ShapeDtypeStruct((2 * len(ORDER) * LINE,), jnp.int32),
        compiler_params=params(4),
        cost_estimate=AHEAD,
        name="plan",
    )()


def edges_kernel(volume, after, cells, inner, outer):
    depth = volume.shape[2]
    core = lax.axis_index("slab") & 1
    for c in range(2):
        turned = volume[:, c, :].T
        cells[c * depth : (c + 1) * depth, :] = turned
        head, tail = turned[:1, :], turned[depth - 1 :, :]
        inner[c : c + 1, :] = jnp.where(core == 0, tail, head)
        outer[c : c + 1, :] = jnp.where(core == 0, head, tail)


def edges(volume, after):
    share, _, depth = volume.shape
    outs = [((2 * depth, share), jnp.float32)] + [((2, share), jnp.float32)] * 2
    return call(edges_kernel, [VMEM, ANY], outs, 1 << 20, 4)(volume, after)


def scale_kernel(table, ids, weights, updates, scaled):
    depth = updates.shape[2]
    for a in range(updates.shape[0]):
        weight = weights[ids[a]]
        for c in range(2):
            at = slice(c * depth, (c + 1) * depth)
            scaled[a, at, :] = (weight * updates[a, c]).astype(jnp.bfloat16)


def scale(updates, table, ids, weights):
    angles, _, depth, detector = updates.shape
    outs = [((angles, 2 * depth, detector), jnp.bfloat16)]
    return call(scale_kernel, [SMEM, SMEM, SMEM, VMEM], outs, 1 << 33, 8)(
        table, ids, weights, updates
    )[0]


def product(sources, tiles, starts, j):
    angles, _, _, block = tiles.shape
    rows = []
    for source in sources:
        windows = []
        for a in range(angles):
            start = pl.multiple_of(starts[a, j] * block, block)
            windows.append(source[a, :, pl.ds(start, 2 * block)])
        rows.append(jnp.concatenate(windows, axis=1))
    weights = jnp.concatenate([tiles[a, j] for a in range(angles)], axis=0)
    return jnp.dot(
        jnp.concatenate(rows, axis=0), weights, preferred_element_type=jnp.float32
    )


PAIR = LINE // 2


def own_kernel(ds, table, starts, scaled, tiles, *outs):
    for d, out in zip(ds, outs):
        for k in range(LINE):
            j = table[place(d) + k]
            out[k] = product((scaled,), tiles, starts, j).astype(out.dtype)


def own_rows(scaled, tiles, table, starts, ds, dtypes):
    angles, _, band, block = tiles.shape
    rows = scaled.shape[1]
    outs = [((LINE, rows, block), dtype) for dtype in dtypes]
    flops = 2 * len(ds) * LINE * angles * rows * band * block
    kernel = functools.partial(own_kernel, ds)
    return call(kernel, [SMEM, SMEM, VMEM, VMEM], outs, flops)(
        table, starts, scaled, tiles
    )


def join_kernel(d, table, starts, other, tiles, own, after, lower, upper):
    rows = other.shape[1]
    for k in range(LINE):
        j = table[place(d) + k]
        out = (lower, upper)[k // PAIR].at[k % PAIR]
        out[:rows, :] = own[k].astype(out.dtype)
        out[rows:, :] = product((other,), tiles, starts, j).astype(out.dtype)


def joined(other, tiles, table, starts, d, dtypes, own, after):
    angles, _, band, block = tiles.shape
    rows = other.shape[1]
    outs = [((PAIR, 2 * rows, block), dtype) for dtype in dtypes]
    flops = 2 * LINE * angles * rows * band * block
    kernel = functools.partial(join_kernel, d)
    specs = [SMEM, SMEM, VMEM, VMEM, VMEM, ANY]
    return call(kernel, specs, outs, flops)(table, starts, other, tiles, own, after)


def both_kernel(d, table, starts, scaled, other, tiles, after, lower, upper):
    for k in range(LINE):
        j = table[place(d) + k]
        out = (lower, upper)[k // PAIR]
        out[k % PAIR] = product((scaled, other), tiles, starts, j).astype(out.dtype)


def both_rows(scaled, other, tiles, table, starts, d, dtypes, after):
    angles, _, band, block = tiles.shape
    rows = 2 * scaled.shape[1]
    outs = [((PAIR, rows, block), dtype) for dtype in dtypes]
    flops = 2 * LINE * angles * rows * band * block
    kernel = functools.partial(both_kernel, d)
    specs = [SMEM, SMEM, VMEM, VMEM, VMEM, ANY]
    return call(kernel, specs, outs, flops)(table, starts, scaled, other, tiles, after)


def add_kernel(own, came, out):
    for k in range(PAIR):
        out[k] = (own[k] + came[k].astype(jnp.float32)).astype(out.dtype)


def added(own, came):
    return call(add_kernel, [VMEM] * 2, [(came.shape, came.dtype)], 1 << 18, 4)(own, came)[0]


def line_kernel(lower, upper, l1, l3, h1, h3, kept, *sent):
    for k in range(LINE):
        own, one, two = ((lower, l1, l3), (upper, h1, h3))[k // PAIR]
        i = k % PAIR
        total = own[i] + one[i].astype(jnp.float32) + two[i].astype(jnp.float32)
        if k == 0:
            kept[...] = total
        else:
            sent[k - 1][...] = total.astype(jnp.bfloat16)


def line_sum(own, arrived):
    tile = own[0].shape[1:]
    outs = [(tile, jnp.float32)] + [(tile, jnp.bfloat16)] * (LINE - 1)
    kept, *sent = call(line_kernel, [VMEM] * 6, outs, 1 << 20)(*own, *arrived)
    return kept, sent


def smooth_kernel(cells, inner, outer, smooth):
    rows, share = cells.shape
    depth = rows // 2
    core = lax.axis_index("slab") & 1
    before = jnp.where(core == 0, outer[...], inner[...])
    after = jnp.where(core == 0, inner[...], outer[...])
    z = lax.broadcasted_iota(jnp.int32, (depth, share), 0)
    for c in range(2):
        at = slice(c * depth, (c + 1) * depth)
        value = cells[at, :]
        down = jnp.where(z == 0, before[c : c + 1, :], pltpu.roll(value, 1, 0))
        up = jnp.where(z == depth - 1, after[c : c + 1, :], pltpu.roll(value, depth - 1, 0))
        smooth[at, :] = value - SMOOTHING * (2.0 * value - down - up)


def smoothed(cells, inner, outer):
    outs = [(cells.shape, jnp.float32)]
    return call(smooth_kernel, [VMEM] * 3, outs, 1 << 20, 4)(cells, inner, outer)[0]


def merge_kernel(smooth, beside, own, s1, s2, s3, mine, message):
    _, zh, _, owner = position()
    rows = smooth.shape[0]
    for at, part in ((slice(0, rows), smooth), (slice(rows, 2 * rows), beside)):
        total = own[at, :]
        for ref in (s1, s2, s3):
            total = total + ref[at, :].astype(jnp.float32)
        total = jnp.where(zh == owner, total + part[...], total)
        mine[at, :] = total
        message[at, :] = total.astype(message.dtype)


def merged(smooth, beside, own, reached):
    outs = [(own.shape, jnp.float32), (own.shape, jnp.bfloat16)]
    return call(merge_kernel, [VMEM] * 6, outs, 1 << 20, 4)(
        smooth, beside, own, *reached
    )


def finish_kernel(mine, crossed, own, beside, lowered):
    rows, _ = own.shape
    depth = rows // 2
    for slab, out in enumerate((own, beside)):
        for c in range(2):
            at = slice(slab * rows + c * depth, slab * rows + (c + 1) * depth)
            value = mine[at, :] + crossed[at, :].astype(jnp.float32)
            if c == 1:
                value = jnp.maximum(value, 0.0)
            out[c * depth : (c + 1) * depth, :] = value
            lowered[at, :] = value.astype(lowered.dtype)


def finished(mine, crossed):
    rows, share = mine.shape
    outs = [((rows // 2, share), jnp.float32)] * 2 + [(mine.shape, jnp.bfloat16)]
    return call(finish_kernel, [VMEM] * 2, outs, 1 << 20, 4)(mine, crossed)


def turn_kernel(own, received, volume, token):
    token[...] = jnp.zeros_like(token)
    _, zh, _, owner = position()
    depth = volume.shape[2]
    for c in range(2):
        at = slice(c * depth, (c + 1) * depth)
        volume[:, c, :] = jnp.where(zh == owner, own[at, :], received[at, :]).T


def turned(own, received, shape):
    outs = [(shape, jnp.float32), ((8, 128), jnp.float32)]
    return call(turn_kernel, [VMEM] * 2, outs, 1 << 20, 4)(own, received)


GROUPS = (0, 1, 3, 2)


def spread_kernel(table, starts, tiles, after, *outs):
    block = tiles.shape[3]
    zeros = jnp.zeros((block, block), tiles.dtype)

    def angle(a, carry):
        for out, d in zip(outs, GROUPS):
            for i in range(2 * LINE):
                half, k = divmod(i, LINE)
                j = table[half * len(ORDER) * LINE + place(d) + k]
                first = starts[a, j]
                column = slice(i * block, (i + 1) * block)
                for empty in (jnp.where(first == 0, 2, 0), jnp.where(first == 2, 1, 3)):
                    at = pl.ds(pl.multiple_of(empty * block, block), block)
                    out[a, at, column] = zeros
                at = pl.ds(pl.multiple_of(first * block, block), 2 * block)
                out[a, at, column] = tiles[a, j]
        return carry

    lax.fori_loop(0, tiles.shape[0], angle, 0)


def spread(tiles, table, starts, detector, after):
    angles, _, _, block = tiles.shape
    outs = [((angles, detector, 2 * LINE * block), tiles.dtype)] * len(GROUPS)
    return call(spread_kernel, [SMEM, SMEM, VMEM, ANY], outs, 1 << 31, 16)(
        table, starts, tiles, after
    )


def cut_kernel(lower, upper, out):
    rows = out.shape[1]
    for k in range(LINE):
        out[k] = (lower, upper)[k // PAIR][k % PAIR, rows:, :]


def cut(lower, upper):
    _, rows, block = lower.shape
    outs = [((LINE, rows // 2, block), lower.dtype)]
    return call(cut_kernel, [VMEM] * 2, outs, 1 << 18, 4)(lower, upper)[0]


def own_blocks(lower, upper):
    rows = lower.shape[1] // 2
    return [(lower, upper)[k // PAIR][k % PAIR, :rows, :] for k in range(LINE)]


def projected(blocks, weights):
    row = jnp.concatenate(blocks, axis=1)
    return lax.dot_general(
        row, weights, (((1,), (1,)), ((), ())), preferred_element_type=jnp.float32
    )


def image_kernel(chained, whole, weights, lower, upper, *refs):
    *refs, after, image = refs
    blocks = own_blocks(lower, upper)
    if whole:
        blocks += [refs[0][k] for k in range(LINE)]
    depth = sum(block.shape[1] for block in blocks)
    for a in range(image.shape[0]):
        value = projected(blocks, weights[a, :, :depth])
        image[a] = refs[-1][a] + value if chained else value


def imaged(weights, piece, got, before, after):
    angles, detector, _ = weights.shape
    rows = piece[0].shape[1] // 2
    more = [v for v in (got, before) if v is not None]
    outs = [((angles, rows, detector), jnp.float32)]
    flops = weights.size * rows * (1 if got is None else 2)
    kernel = functools.partial(image_kernel, before is not None, got is not None)
    specs = [VMEM] * (3 + len(more)) + [ANY]
    return call(kernel, specs, outs, flops)(weights, *piece, *more, after)[0]


def leave_kernel(weights, got, before, out, image, done):
    blocks = [got[k] for k in range(LINE)]
    depth = sum(block.shape[1] for block in blocks)
    copies = []
    for a in range(image.shape[0]):
        image[a] = before[a] + projected(blocks, weights[a, :, depth:])
        copies.append(pltpu.make_async_copy(image.at[a], out.at[a], done.at[a]))
        copies[-1].start()
    for copy in copies:
        copy.wait()


def leave(weights, got, before):
    shape = before.shape
    return pl.pallas_call(
        leave_kernel,
        in_specs=[VMEM] * 3,
        out_specs=ANY,
        out_shape=jax.ShapeDtypeStruct(shape, jnp.float32),
        scratch_shapes=[pltpu.VMEM(shape, jnp.float32), pltpu.SemaphoreType.DMA((shape[0],))],
        compiler_params=params(16),
        cost_estimate=pl.CostEstimate(flops=1 << 28, bytes_accessed=1 << 20, transcendentals=0),
        name="leave",
    )(weights, got, before)


def steps(updates, tiles, starts, ids, weights, volume):
    angles, _, depth, detector = updates.shape
    count = lax.axis_size("slab")
    table = plan()
    scaled = scale(updates, table, ids, weights)
    other = swapped(scaled)
    cells, inner, outer = edges(volume, scaled)
    inner = swapped(inner)
    odd = range(1, count - 1, 2)
    outer = lax.ppermute(outer, "slab", [p for i in odd for p in ((i, i + 1), (i + 1, i))])
    bf, wide = jnp.bfloat16, jnp.float32
    own2, own1 = own_rows(scaled, tiles, table, starts, (2, 1), (bf, wide))
    low2, up2 = joined(other, tiles, table, starts, 2, (bf, bf), own2, own1)
    low1, up1 = joined(other, tiles, table, starts, 1, (wide, bf), own1, low2)
    low3, up3 = both_rows(scaled, other, tiles, table, starts, 3, (bf, wide), up1)
    own = both_rows(scaled, other, tiles, table, starts, 0, (wide, wide), low3)
    low2 = moved(low2, True, 1)
    up2 = moved(up2, True, -1)
    up1 = moved(up1, True, 1)
    low3 = moved(low3, True, -1)
    low1, up3 = added(low1, low2), added(up3, up2)
    low1 = moved(low1, True, 1)
    up3 = moved(up3, True, -1)
    kept, passed = line_sum(own, (low1, low3, up1, up3))
    reached = []
    for d in FAR:
        reached.append(moved(passed[d - 1], False, d))
    smooth = smoothed(cells, inner, outer)
    beside = swapped(smooth)
    mine, message = merged(smooth, beside, kept, reached)
    crossed = across(message)
    bands = dict(zip(GROUPS, spread(tiles, table, starts, detector, message)))
    own, beside, lowered = finished(mine, crossed)

    came = {}
    for d in FAR:
        came[d] = moved(lowered, False, LINE - d)
    beside, came[1], came[2], came[3] = lax.optimization_barrier(
        (beside, came[1], came[2], came[3])
    )
    pieces = {0: (jnp.stack([lowered, came[1]]), jnp.stack([came[2], came[3]]))}
    lower, upper = pieces[0]
    low1 = moved(lower, True, -1)
    up3 = moved(upper, True, 1)
    up1 = moved(upper, True, -1)
    low3 = moved(lower, True, 1)
    low2 = moved(low1, True, -1)
    up2 = moved(up3, True, 1)
    pieces |= {1: (low1, up1), 3: (low3, up3), 2: (low2, up2)}
    received = swapped(beside)
    volume_next, token = turned(own, received, volume.shape)
    image, last = None, token
    for d in GROUPS:
        got = swapped(cut(*pieces[d]))
        whole = None if d == GROUPS[-1] else got
        image = imaged(bands[d], pieces[d], whole, image, last)
        last = image
    projection = leave(bands[GROUPS[-1]], got, image)
    return volume_next, projection.reshape(angles, 2, depth, detector)


def solution(mesh):
    placed = (
        P("ang", None, "slab", None),
        P("ang", None, None, None),
        P("ang", None),
        P("ang"),
        P(),
        P("ang", None, "slab"),
    )
    return jax.shard_map(
        steps,
        mesh=mesh,
        in_specs=placed,
        out_specs=(P("ang", None, "slab"), P("ang", None, "slab", None)),
        check_vma=False,
    )
```

```python
import functools

import jax
import jax.numpy as jnp
from jax import lax
from jax.experimental import pallas as pl
from jax.experimental.pallas import tpu as pltpu
from jax.sharding import PartitionSpec as P


SMOOTHING = 0.25
YS, ZS, XS, SLABS = 4, 2, 4, 8
LINE = 4
FAR = (2, 1, 3)
ORDER = (*FAR, 0)


def position():
    me, core = lax.axis_index("ang"), lax.axis_index("slab") & 1
    y, zh, x = lax.shift_right_logical(me, 3), lax.shift_right_logical(me, 2) & 1, me & 3
    return y, zh, x, 1 - core


def moved(value, first, delta):
    pairs = []
    for y in range(YS):
        for zh in range(ZS):
            for x in range(XS):
                for slab in range(SLABS):
                    along_x = (slab % 2 == 1) == first
                    ty, tx = (y, (x + delta) % XS) if along_x else ((y + delta) % YS, x)
                    source, target = (y * ZS + zh) * XS + x, (ty * ZS + zh) * XS + tx
                    pairs.append((source * SLABS + slab, target * SLABS + slab))
    return lax.ppermute(value, ("ang", "slab"), pairs)


def across(value):
    return lax.ppermute(value, "ang", [(a, a ^ XS) for a in range(YS * ZS * XS)])


def swapped(value):
    return lax.ppermute(value, "slab", [(i, i ^ 1) for i in range(SLABS)])


def place(d):
    return ORDER.index(d) * LINE


def params(mib, **more):
    return pltpu.CompilerParams(vmem_limit_bytes=mib << 20, **more)


VMEM = pl.BlockSpec(memory_space=pltpu.VMEM)
SMEM = pl.BlockSpec(memory_space=pltpu.SMEM)
ANY = pl.BlockSpec(memory_space=pl.ANY)
AHEAD = pl.CostEstimate(flops=1 << 33, bytes_accessed=1 << 20, transcendentals=0)


def call(kernel, in_specs, outs, flops, mib=16):
    return pl.pallas_call(
        kernel,
        in_specs=in_specs,
        out_specs=[VMEM] * len(outs),
        out_shape=[jax.ShapeDtypeStruct(shape, dtype) for shape, dtype in outs],
        compiler_params=params(mib),
        cost_estimate=pl.CostEstimate(flops=flops, bytes_accessed=1 << 20, transcendentals=0),
    )


def plan_kernel(table):
    y, _, x, own = position()
    for half, owner in enumerate((own, 1 - own)):
        for i, (d, k) in enumerate((d, k) for d in ORDER for k in range(LINE)):
            dy = k + owner * (d - k)
            dx = d + owner * (k - d)
            at = half * len(ORDER) * LINE + i
            table[at] = ((y + dy) & 3) * 8 + owner * 4 + ((x + dx) & 3)


def plan():
    return pl.pallas_call(
        plan_kernel,
        out_specs=SMEM,
        out_shape=jax.ShapeDtypeStruct((2 * len(ORDER) * LINE,), jnp.int32),
        compiler_params=params(4),
        cost_estimate=AHEAD,
        name="plan",
    )()


def edges_kernel(volume, after, cells, inner, outer):
    depth = volume.shape[2]
    core = lax.axis_index("slab") & 1
    for c in range(2):
        turned = volume[:, c, :].T
        cells[c * depth : (c + 1) * depth, :] = turned
        head, tail = turned[:1, :], turned[depth - 1 :, :]
        inner[c : c + 1, :] = jnp.where(core == 0, tail, head)
        outer[c : c + 1, :] = jnp.where(core == 0, head, tail)


def edges(volume, after):
    share, _, depth = volume.shape
    outs = [((2 * depth, share), jnp.float32)] + [((2, share), jnp.float32)] * 2
    return call(edges_kernel, [VMEM, ANY], outs, 1 << 20, 4)(volume, after)


def scale_kernel(table, ids, weights, updates, scaled):
    depth = updates.shape[2]
    for a in range(updates.shape[0]):
        weight = weights[ids[a]]
        for c in range(2):
            at = slice(c * depth, (c + 1) * depth)
            scaled[a, at, :] = (weight * updates[a, c]).astype(jnp.bfloat16)


def scale(updates, table, ids, weights):
    angles, _, depth, detector = updates.shape
    outs = [((angles, 2 * depth, detector), jnp.bfloat16)]
    return call(scale_kernel, [SMEM, SMEM, SMEM, VMEM], outs, 1 << 33, 8)(
        table, ids, weights, updates
    )[0]


def product(sources, tiles, starts, j):
    angles, _, _, block = tiles.shape
    rows = []
    for source in sources:
        windows = []
        for a in range(angles):
            start = pl.multiple_of(starts[a, j] * block, block)
            windows.append(source[a, :, pl.ds(start, 2 * block)])
        rows.append(jnp.concatenate(windows, axis=1))
    weights = jnp.concatenate([tiles[a, j] for a in range(angles)], axis=0)
    return jnp.dot(
        jnp.concatenate(rows, axis=0), weights, preferred_element_type=jnp.float32
    )


def own_kernel(ds, table, starts, scaled, tiles, *outs):
    for d, out in zip(ds, outs):
        for k in range(LINE):
            j = table[place(d) + k]
            out[k] = product((scaled,), tiles, starts, j).astype(out.dtype)


def own_rows(scaled, tiles, table, starts, ds):
    angles, _, band, block = tiles.shape
    rows = scaled.shape[1]
    outs = [((LINE, rows, block), jnp.bfloat16)] * len(ds)
    flops = 2 * len(ds) * LINE * angles * rows * band * block
    kernel = functools.partial(own_kernel, ds)
    return call(kernel, [SMEM, SMEM, VMEM, VMEM], outs, flops)(
        table, starts, scaled, tiles
    )


def join_kernel(d, table, starts, other, tiles, own, after, out):
    rows = other.shape[1]
    for k in range(LINE):
        j = table[place(d) + k]
        out[k, :rows, :] = own[k]
        out[k, rows:, :] = product((other,), tiles, starts, j).astype(out.dtype)


def joined(other, tiles, table, starts, d, own, after):
    angles, _, band, block = tiles.shape
    rows = other.shape[1]
    outs = [((LINE, 2 * rows, block), jnp.bfloat16)]
    flops = 2 * LINE * angles * rows * band * block
    kernel = functools.partial(join_kernel, d)
    specs = [SMEM, SMEM, VMEM, VMEM, VMEM, ANY]
    return call(kernel, specs, outs, flops)(table, starts, other, tiles, own, after)[0]


def both_kernel(d, table, starts, scaled, other, tiles, after, out):
    for k in range(LINE):
        j = table[place(d) + k]
        out[k] = product((scaled, other), tiles, starts, j).astype(out.dtype)


def both_rows(scaled, other, tiles, table, starts, d, dtype, after):
    angles, _, band, block = tiles.shape
    rows = 2 * scaled.shape[1]
    flops = 2 * LINE * angles * rows * band * block
    kernel = functools.partial(both_kernel, d)
    specs = [SMEM, SMEM, VMEM, VMEM, VMEM, ANY]
    return call(kernel, specs, [((LINE, rows, block), dtype)], flops)(
        table, starts, scaled, other, tiles, after
    )[0]


def line_kernel(own, s1, s2, s3, kept, *sent):
    for k in range(LINE):
        total = own[k]
        for ref in (s1, s2, s3):
            total = total + ref[k].astype(jnp.float32)
        if k == 0:
            kept[...] = total
        else:
            sent[k - 1][...] = total.astype(jnp.bfloat16)


def line_sum(own, arrived):
    tile = own.shape[1:]
    outs = [(tile, jnp.float32)] + [(tile, jnp.bfloat16)] * (LINE - 1)
    kept, *sent = call(line_kernel, [VMEM] * 4, outs, 1 << 20)(own, *arrived)
    return kept, sent


def smooth_kernel(cells, inner, outer, smooth):
    rows, share = cells.shape
    depth = rows // 2
    core = lax.axis_index("slab") & 1
    before = jnp.where(core == 0, outer[...], inner[...])
    after = jnp.where(core == 0, inner[...], outer[...])
    z = lax.broadcasted_iota(jnp.int32, (depth, share), 0)
    for c in range(2):
        at = slice(c * depth, (c + 1) * depth)
        value = cells[at, :]
        down = jnp.where(z == 0, before[c : c + 1, :], pltpu.roll(value, 1, 0))
        up = jnp.where(z == depth - 1, after[c : c + 1, :], pltpu.roll(value, depth - 1, 0))
        smooth[at, :] = value - SMOOTHING * (2.0 * value - down - up)


def smoothed(cells, inner, outer):
    outs = [(cells.shape, jnp.float32)]
    return call(smooth_kernel, [VMEM] * 3, outs, 1 << 20, 4)(cells, inner, outer)[0]


def merge_kernel(smooth, beside, own, s1, s2, s3, mine, message):
    _, zh, _, owner = position()
    rows = smooth.shape[0]
    for at, part in ((slice(0, rows), smooth), (slice(rows, 2 * rows), beside)):
        total = own[at, :]
        for ref in (s1, s2, s3):
            total = total + ref[at, :].astype(jnp.float32)
        total = jnp.where(zh == owner, total + part[...], total)
        mine[at, :] = total
        message[at, :] = total.astype(message.dtype)


def merged(smooth, beside, own, reached):
    outs = [(own.shape, jnp.float32), (own.shape, jnp.bfloat16)]
    return call(merge_kernel, [VMEM] * 6, outs, 1 << 20, 4)(
        smooth, beside, own, *reached
    )


def finish_kernel(mine, crossed, own, beside, lowered):
    rows, _ = own.shape
    depth = rows // 2
    for slab, out in enumerate((own, beside)):
        for c in range(2):
            at = slice(slab * rows + c * depth, slab * rows + (c + 1) * depth)
            value = mine[at, :] + crossed[at, :].astype(jnp.float32)
            if c == 1:
                value = jnp.maximum(value, 0.0)
            out[c * depth : (c + 1) * depth, :] = value
            lowered[at, :] = value.astype(lowered.dtype)


def finished(mine, crossed):
    rows, share = mine.shape
    outs = [((rows // 2, share), jnp.float32)] * 2 + [(mine.shape, jnp.bfloat16)]
    return call(finish_kernel, [VMEM] * 2, outs, 1 << 20, 4)(mine, crossed)


def turn_kernel(own, received, volume, token):
    token[...] = jnp.zeros_like(token)
    _, zh, _, owner = position()
    depth = volume.shape[2]
    for c in range(2):
        at = slice(c * depth, (c + 1) * depth)
        volume[:, c, :] = jnp.where(zh == owner, own[at, :], received[at, :]).T


def turned(own, received, shape):
    outs = [(shape, jnp.float32), ((8, 128), jnp.float32)]
    return call(turn_kernel, [VMEM] * 2, outs, 1 << 20, 4)(own, received)


GROUPS = (0, *FAR)


def spread_kernel(table, starts, tiles, after, *outs):
    block = tiles.shape[3]
    zeros = jnp.zeros((block, block), tiles.dtype)

    def angle(a, carry):
        for out, d in zip(outs, GROUPS):
            for i in range(2 * LINE):
                half, k = divmod(i, LINE)
                j = table[half * len(ORDER) * LINE + place(d) + k]
                first = starts[a, j]
                column = slice(i * block, (i + 1) * block)
                for empty in (jnp.where(first == 0, 2, 0), jnp.where(first == 2, 1, 3)):
                    at = pl.ds(pl.multiple_of(empty * block, block), block)
                    out[a, at, column] = zeros
                at = pl.ds(pl.multiple_of(first * block, block), 2 * block)
                out[a, at, column] = tiles[a, j]
        return carry

    lax.fori_loop(0, tiles.shape[0], angle, 0)


def spread(tiles, table, starts, detector, after):
    angles, _, _, block = tiles.shape
    outs = [((angles, detector, 2 * LINE * block), tiles.dtype)] * len(GROUPS)
    return call(spread_kernel, [SMEM, SMEM, VMEM, ANY], outs, 1 << 31, 16)(
        table, starts, tiles, after
    )


def cut_kernel(piece, out):
    out[...] = piece[:, out.shape[1] :, :]


def cut(piece):
    count, rows, block = piece.shape
    outs = [((count, rows // 2, block), piece.dtype)]
    return call(cut_kernel, [VMEM], outs, 1 << 18, 4)(piece)[0]


def projected(blocks, weights):
    row = jnp.concatenate(blocks, axis=1)
    return lax.dot_general(
        row, weights, (((1,), (1,)), ((), ())), preferred_element_type=jnp.float32
    )


def image_kernel(chained, whole, weights, piece, *refs):
    *refs, after, image = refs
    blocks = [piece[k, : piece.shape[1] // 2, :] for k in range(LINE)]
    if whole:
        blocks += [refs[0][k] for k in range(LINE)]
    depth = sum(block.shape[1] for block in blocks)
    for a in range(image.shape[0]):
        value = projected(blocks, weights[a, :, :depth])
        image[a] = refs[-1][a] + value if chained else value


def imaged(weights, piece, got, before, after):
    angles, detector, _ = weights.shape
    rows = piece.shape[1] // 2
    more = [v for v in (got, before) if v is not None]
    outs = [((angles, rows, detector), jnp.float32)]
    flops = weights.size * rows * (1 if got is None else 2)
    kernel = functools.partial(image_kernel, before is not None, got is not None)
    specs = [VMEM] * (2 + len(more)) + [ANY]
    return call(kernel, specs, outs, flops)(weights, piece, *more, after)[0]


def leave_kernel(weights, got, before, out, image, done):
    blocks = [got[k] for k in range(LINE)]
    depth = sum(block.shape[1] for block in blocks)
    copies = []
    for a in range(image.shape[0]):
        image[a] = before[a] + projected(blocks, weights[a, :, depth:])
        copies.append(pltpu.make_async_copy(image.at[a], out.at[a], done.at[a]))
        copies[-1].start()
    for copy in copies:
        copy.wait()


def leave(weights, got, before):
    shape = before.shape
    return pl.pallas_call(
        leave_kernel,
        in_specs=[VMEM] * 3,
        out_specs=ANY,
        out_shape=jax.ShapeDtypeStruct(shape, jnp.float32),
        scratch_shapes=[pltpu.VMEM(shape, jnp.float32), pltpu.SemaphoreType.DMA((shape[0],))],
        compiler_params=params(16),
        cost_estimate=pl.CostEstimate(flops=1 << 28, bytes_accessed=1 << 20, transcendentals=0),
        name="leave",
    )(weights, got, before)


def steps(updates, tiles, starts, ids, weights, volume):
    angles, _, depth, detector = updates.shape
    count = lax.axis_size("slab")
    table = plan()
    scaled = scale(updates, table, ids, weights)
    other = swapped(scaled)
    own2, own1 = own_rows(scaled, tiles, table, starts, (2, 1))
    sent = {}
    sent[2] = joined(other, tiles, table, starts, 2, own2, own1)
    sent[1] = joined(other, tiles, table, starts, 1, own1, sent[2])
    sent[3] = both_rows(scaled, other, tiles, table, starts, 3, jnp.bfloat16, sent[1])
    own = both_rows(scaled, other, tiles, table, starts, 0, jnp.float32, sent[3])
    arrived = []
    for d in FAR:
        arrived.append(moved(sent[d], True, d))

    cells, inner, outer = edges(volume, own)
    inner = swapped(inner)
    odd = range(1, count - 1, 2)
    outer = lax.ppermute(outer, "slab", [p for i in odd for p in ((i, i + 1), (i + 1, i))])
    smooth = smoothed(cells, inner, outer)
    beside = swapped(smooth)
    kept, passed = line_sum(own, arrived)
    reached = []
    for d in FAR:
        reached.append(moved(passed[d - 1], False, d))
    mine, message = merged(smooth, beside, kept, reached)
    crossed = across(message)
    bands = dict(zip(GROUPS, spread(tiles, table, starts, detector, message)))
    own, beside, lowered = finished(mine, crossed)

    came = {}
    for d in FAR:
        came[d] = moved(lowered, False, LINE - d)
    beside, came[1], came[2], came[3] = lax.optimization_barrier(
        (beside, came[1], came[2], came[3])
    )
    pieces = {0: jnp.stack([lowered] + [came[d] for d in range(1, LINE)])}
    for d in FAR:
        pieces[d] = moved(pieces[0], True, LINE - d)
    received = swapped(beside)
    volume_next, token = turned(own, received, volume.shape)
    image, last = None, token
    for d in GROUPS:
        got = swapped(cut(pieces[d]))
        whole = None if d == FAR[-1] else got
        image = imaged(bands[d], pieces[d], whole, image, last)
        last = image
    projection = leave(bands[FAR[-1]], got, image)
    return volume_next, projection.reshape(angles, 2, depth, detector)


def solution(mesh):
    placed = (
        P("ang", None, "slab", None),
        P("ang", None, None, None),
        P("ang", None),
        P("ang"),
        P(),
        P("ang", None, "slab"),
    )
    return jax.shard_map(
        steps,
        mesh=mesh,
        in_specs=placed,
        out_specs=(P("ang", None, "slab"), P("ang", None, "slab", None)),
        check_vma=False,
    )
```

```python
import functools

import jax
import jax.numpy as jnp
from jax import lax
from jax.experimental import pallas as pl
from jax.experimental.pallas import tpu as pltpu
from jax.sharding import PartitionSpec as P


SMOOTHING = 0.25
YS, ZS, XS, SLABS = 4, 2, 4, 8
LINE = 4
FAR = (2, 1, 3)
ORDER = (*FAR, 0)


def position():
    me, core = lax.axis_index("ang"), lax.axis_index("slab") & 1
    y, zh, x = lax.shift_right_logical(me, 3), lax.shift_right_logical(me, 2) & 1, me & 3
    return y, zh, x, 1 - core


def moved(value, first, delta):
    pairs = []
    for y in range(YS):
        for zh in range(ZS):
            for x in range(XS):
                for slab in range(SLABS):
                    along_x = (slab % 2 == 1) == first
                    ty, tx = (y, (x + delta) % XS) if along_x else ((y + delta) % YS, x)
                    source, target = (y * ZS + zh) * XS + x, (ty * ZS + zh) * XS + tx
                    pairs.append((source * SLABS + slab, target * SLABS + slab))
    return lax.ppermute(value, ("ang", "slab"), pairs)


def across(value):
    return lax.ppermute(value, "ang", [(a, a ^ XS) for a in range(YS * ZS * XS)])


def swapped(value):
    return lax.ppermute(value, "slab", [(i, i ^ 1) for i in range(SLABS)])


def place(d):
    return ORDER.index(d) * LINE


def params(mib, **more):
    return pltpu.CompilerParams(vmem_limit_bytes=mib << 20, **more)


VMEM = pl.BlockSpec(memory_space=pltpu.VMEM)
SMEM = pl.BlockSpec(memory_space=pltpu.SMEM)
ANY = pl.BlockSpec(memory_space=pl.ANY)
AHEAD = pl.CostEstimate(flops=1 << 33, bytes_accessed=1 << 20, transcendentals=0)


def call(kernel, in_specs, outs, flops, mib=16):
    return pl.pallas_call(
        kernel,
        in_specs=in_specs,
        out_specs=[VMEM] * len(outs),
        out_shape=[jax.ShapeDtypeStruct(shape, dtype) for shape, dtype in outs],
        compiler_params=params(mib),
        cost_estimate=pl.CostEstimate(flops=flops, bytes_accessed=1 << 20, transcendentals=0),
    )


def plan_kernel(table):
    y, _, x, own = position()
    for half, owner in enumerate((own, 1 - own)):
        for i, (d, k) in enumerate((d, k) for d in ORDER for k in range(LINE)):
            dy = k + owner * (d - k)
            dx = d + owner * (k - d)
            at = half * len(ORDER) * LINE + i
            table[at] = ((y + dy) & 3) * 8 + owner * 4 + ((x + dx) & 3)


def plan():
    return pl.pallas_call(
        plan_kernel,
        out_specs=SMEM,
        out_shape=jax.ShapeDtypeStruct((2 * len(ORDER) * LINE,), jnp.int32),
        compiler_params=params(4),
        cost_estimate=AHEAD,
        name="plan",
    )()


def edges_kernel(volume, after, cells, inner, outer):
    depth = volume.shape[2]
    core = lax.axis_index("slab") & 1
    for c in range(2):
        turned = volume[:, c, :].T
        cells[c * depth : (c + 1) * depth, :] = turned
        head, tail = turned[:1, :], turned[depth - 1 :, :]
        inner[c : c + 1, :] = jnp.where(core == 0, tail, head)
        outer[c : c + 1, :] = jnp.where(core == 0, head, tail)


def edges(volume, after):
    share, _, depth = volume.shape
    outs = [((2 * depth, share), jnp.float32)] + [((2, share), jnp.float32)] * 2
    return call(edges_kernel, [VMEM, ANY], outs, 1 << 20, 4)(volume, after)


def scale_kernel(table, ids, weights, updates, scaled):
    depth = updates.shape[2]
    for a in range(updates.shape[0]):
        weight = weights[ids[a]]
        for c in range(2):
            at = slice(c * depth, (c + 1) * depth)
            scaled[a, at, :] = (weight * updates[a, c]).astype(jnp.bfloat16)


def scale(updates, table, ids, weights):
    angles, _, depth, detector = updates.shape
    outs = [((angles, 2 * depth, detector), jnp.bfloat16)]
    return call(scale_kernel, [SMEM, SMEM, SMEM, VMEM], outs, 1 << 33, 8)(
        table, ids, weights, updates
    )[0]


def product(sources, tiles, starts, j):
    angles, _, _, block = tiles.shape
    rows = []
    for source in sources:
        windows = []
        for a in range(angles):
            start = pl.multiple_of(starts[a, j] * block, block)
            windows.append(source[a, :, pl.ds(start, 2 * block)])
        rows.append(jnp.concatenate(windows, axis=1))
    weights = jnp.concatenate([tiles[a, j] for a in range(angles)], axis=0)
    return jnp.dot(
        jnp.concatenate(rows, axis=0), weights, preferred_element_type=jnp.float32
    )


def own_kernel(ds, table, starts, scaled, tiles, *outs):
    for d, out in zip(ds, outs):
        for k in range(LINE):
            j = table[place(d) + k]
            out[k] = product((scaled,), tiles, starts, j).astype(out.dtype)


def own_rows(scaled, tiles, table, starts, ds):
    angles, _, band, block = tiles.shape
    rows = scaled.shape[1]
    outs = [((LINE, rows, block), jnp.bfloat16)] * len(ds)
    flops = 2 * len(ds) * LINE * angles * rows * band * block
    kernel = functools.partial(own_kernel, ds)
    return call(kernel, [SMEM, SMEM, VMEM, VMEM], outs, flops)(
        table, starts, scaled, tiles
    )


def join_kernel(d, table, starts, other, tiles, own, after, out):
    rows = other.shape[1]
    for k in range(LINE):
        j = table[place(d) + k]
        out[k, :rows, :] = own[k]
        out[k, rows:, :] = product((other,), tiles, starts, j).astype(out.dtype)


def joined(other, tiles, table, starts, d, own, after):
    angles, _, band, block = tiles.shape
    rows = other.shape[1]
    outs = [((LINE, 2 * rows, block), jnp.bfloat16)]
    flops = 2 * LINE * angles * rows * band * block
    kernel = functools.partial(join_kernel, d)
    specs = [SMEM, SMEM, VMEM, VMEM, VMEM, ANY]
    return call(kernel, specs, outs, flops)(table, starts, other, tiles, own, after)[0]


def both_kernel(d, table, starts, scaled, other, tiles, after, out):
    for k in range(LINE):
        j = table[place(d) + k]
        out[k] = product((scaled, other), tiles, starts, j).astype(out.dtype)


def both_rows(scaled, other, tiles, table, starts, d, dtype, after):
    angles, _, band, block = tiles.shape
    rows = 2 * scaled.shape[1]
    flops = 2 * LINE * angles * rows * band * block
    kernel = functools.partial(both_kernel, d)
    specs = [SMEM, SMEM, VMEM, VMEM, VMEM, ANY]
    return call(kernel, specs, [((LINE, rows, block), dtype)], flops)(
        table, starts, scaled, other, tiles, after
    )[0]


def line_kernel(own, s1, s2, s3, kept, *sent):
    for k in range(LINE):
        total = own[k]
        for ref in (s1, s2, s3):
            total = total + ref[k].astype(jnp.float32)
        if k == 0:
            kept[...] = total
        else:
            sent[k - 1][...] = total.astype(jnp.bfloat16)


def line_sum(own, arrived):
    tile = own.shape[1:]
    outs = [(tile, jnp.float32)] + [(tile, jnp.bfloat16)] * (LINE - 1)
    kept, *sent = call(line_kernel, [VMEM] * 4, outs, 1 << 20)(own, *arrived)
    return kept, sent


def smooth_kernel(cells, inner, outer, smooth):
    rows, share = cells.shape
    depth = rows // 2
    core = lax.axis_index("slab") & 1
    before = jnp.where(core == 0, outer[...], inner[...])
    after = jnp.where(core == 0, inner[...], outer[...])
    z = lax.broadcasted_iota(jnp.int32, (depth, share), 0)
    for c in range(2):
        at = slice(c * depth, (c + 1) * depth)
        value = cells[at, :]
        down = jnp.where(z == 0, before[c : c + 1, :], pltpu.roll(value, 1, 0))
        up = jnp.where(z == depth - 1, after[c : c + 1, :], pltpu.roll(value, depth - 1, 0))
        smooth[at, :] = value - SMOOTHING * (2.0 * value - down - up)


def smoothed(cells, inner, outer):
    outs = [(cells.shape, jnp.float32)]
    return call(smooth_kernel, [VMEM] * 3, outs, 1 << 20, 4)(cells, inner, outer)[0]


def merge_kernel(smooth, beside, own, s1, s2, s3, mine, message):
    _, zh, _, owner = position()
    rows = smooth.shape[0]
    for at, part in ((slice(0, rows), smooth), (slice(rows, 2 * rows), beside)):
        total = own[at, :]
        for ref in (s1, s2, s3):
            total = total + ref[at, :].astype(jnp.float32)
        total = jnp.where(zh == owner, total + part[...], total)
        mine[at, :] = total
        message[at, :] = total.astype(message.dtype)


def merged(smooth, beside, own, reached):
    outs = [(own.shape, jnp.float32), (own.shape, jnp.bfloat16)]
    return call(merge_kernel, [VMEM] * 6, outs, 1 << 20, 4)(
        smooth, beside, own, *reached
    )


def finish_kernel(mine, crossed, own, beside, lowered):
    rows, _ = own.shape
    depth = rows // 2
    for slab, out in enumerate((own, beside)):
        for c in range(2):
            at = slice(slab * rows + c * depth, slab * rows + (c + 1) * depth)
            value = mine[at, :] + crossed[at, :].astype(jnp.float32)
            if c == 1:
                value = jnp.maximum(value, 0.0)
            out[c * depth : (c + 1) * depth, :] = value
            lowered[at, :] = value.astype(lowered.dtype)


def finished(mine, crossed):
    rows, share = mine.shape
    outs = [((rows // 2, share), jnp.float32)] * 2 + [(mine.shape, jnp.bfloat16)]
    return call(finish_kernel, [VMEM] * 2, outs, 1 << 20, 4)(mine, crossed)


def turn_kernel(own, received, volume, token):
    token[...] = jnp.zeros_like(token)
    _, zh, _, owner = position()
    depth = volume.shape[2]
    for c in range(2):
        at = slice(c * depth, (c + 1) * depth)
        volume[:, c, :] = jnp.where(zh == owner, own[at, :], received[at, :]).T


def turned(own, received, shape):
    outs = [(shape, jnp.float32), ((8, 128), jnp.float32)]
    return call(turn_kernel, [VMEM] * 2, outs, 1 << 20, 4)(own, received)


COLUMNS = (((0, 0), (1, 0)), ((0, 2), (1, 2)), ((0, 1), (0, 3)), ((1, 1), (1, 3)))


def spread_kernel(table, starts, tiles, after, *outs):
    block = tiles.shape[3]
    zeros = jnp.zeros((block, block), tiles.dtype)

    def angle(a, carry):
        for out, groups in zip(outs, COLUMNS):
            for i in range(2 * LINE):
                half, d = groups[i // LINE]
                j = table[half * len(ORDER) * LINE + place(d) + i % LINE]
                first = starts[a, j]
                column = slice(i * block, (i + 1) * block)
                for empty in (jnp.where(first == 0, 2, 0), jnp.where(first == 2, 1, 3)):
                    at = pl.ds(pl.multiple_of(empty * block, block), block)
                    out[a, at, column] = zeros
                at = pl.ds(pl.multiple_of(first * block, block), 2 * block)
                out[a, at, column] = tiles[a, j]
        return carry

    lax.fori_loop(0, tiles.shape[0], angle, 0)


def spread(tiles, table, starts, detector, after):
    angles, _, _, block = tiles.shape
    outs = [((angles, detector, 2 * LINE * block), tiles.dtype)] * len(COLUMNS)
    return call(spread_kernel, [SMEM, SMEM, VMEM, ANY], outs, 1 << 31, 16)(
        table, starts, tiles, after
    )


def cut_kernel(piece, out):
    out[...] = piece[:, out.shape[1] :, :]


def cut(piece):
    count, rows, block = piece.shape
    outs = [((count, rows // 2, block), piece.dtype)]
    return call(cut_kernel, [VMEM], outs, 1 << 18, 4)(piece)[0]


def projected(blocks, weights):
    row = jnp.concatenate(blocks, axis=1)
    return lax.dot_general(
        row, weights, (((1,), (1,)), ((), ())), preferred_element_type=jnp.float32
    )


def image_kernel(chained, weights, one, two, *refs):
    *refs, after, image = refs
    rows = image.shape[1]
    blocks = [piece[k, :rows, :] for piece in (one, two) for k in range(LINE)]
    for a in range(image.shape[0]):
        value = projected(blocks, weights[a])
        image[a] = refs[0][a] + value if chained else value


def imaged(weights, one, two, before, after):
    angles, detector, _ = weights.shape
    rows = one.shape[1] // 2
    more = [] if before is None else [before]
    outs = [((angles, rows, detector), jnp.float32)]
    kernel = functools.partial(image_kernel, before is not None)
    specs = [VMEM] * (3 + len(more)) + [ANY]
    return call(kernel, specs, outs, 2 * weights.size * rows)(weights, one, two, *more, after)[0]


def leave_kernel(weights, one, two, before, out, image, done):
    blocks = [piece[k] for piece in (one, two) for k in range(LINE)]
    copies = []
    for a in range(image.shape[0]):
        image[a] = before[a] + projected(blocks, weights[a])
        copies.append(pltpu.make_async_copy(image.at[a], out.at[a], done.at[a]))
        copies[-1].start()
    for copy in copies:
        copy.wait()


def leave(weights, one, two, before):
    shape = before.shape
    return pl.pallas_call(
        leave_kernel,
        in_specs=[VMEM] * 4,
        out_specs=ANY,
        out_shape=jax.ShapeDtypeStruct(shape, jnp.float32),
        scratch_shapes=[pltpu.VMEM(shape, jnp.float32), pltpu.SemaphoreType.DMA((shape[0],))],
        compiler_params=params(16),
        cost_estimate=pl.CostEstimate(flops=1 << 29, bytes_accessed=1 << 20, transcendentals=0),
        name="leave",
    )(weights, one, two, before)


def steps(updates, tiles, starts, ids, weights, volume):
    angles, _, depth, detector = updates.shape
    count = lax.axis_size("slab")
    table = plan()
    scaled = scale(updates, table, ids, weights)
    other = swapped(scaled)
    own2, own1 = own_rows(scaled, tiles, table, starts, (2, 1))
    sent = {}
    sent[2] = joined(other, tiles, table, starts, 2, own2, own1)
    sent[1] = joined(other, tiles, table, starts, 1, own1, sent[2])
    sent[3] = both_rows(scaled, other, tiles, table, starts, 3, jnp.bfloat16, sent[1])
    own = both_rows(scaled, other, tiles, table, starts, 0, jnp.float32, sent[3])
    arrived = []
    for d in FAR:
        arrived.append(moved(sent[d], True, d))

    cells, inner, outer = edges(volume, own)
    inner = swapped(inner)
    odd = range(1, count - 1, 2)
    outer = lax.ppermute(outer, "slab", [p for i in odd for p in ((i, i + 1), (i + 1, i))])
    smooth = smoothed(cells, inner, outer)
    beside = swapped(smooth)
    kept, passed = line_sum(own, arrived)
    reached = []
    for d in FAR:
        reached.append(moved(passed[d - 1], False, d))
    mine, message = merged(smooth, beside, kept, reached)
    crossed = across(message)
    bands = spread(tiles, table, starts, detector, message)
    own, beside, lowered = finished(mine, crossed)

    came = {}
    for d in FAR:
        came[d] = moved(lowered, False, LINE - d)
    beside, came[1], came[2], came[3] = lax.optimization_barrier(
        (beside, came[1], came[2], came[3])
    )
    pieces = {0: jnp.stack([lowered] + [came[d] for d in range(1, LINE)])}
    for d in FAR:
        pieces[d] = moved(pieces[0], True, LINE - d)
    received = swapped(beside)
    volume_next, token = turned(own, received, volume.shape)
    got = {}
    for d in (0, *FAR):
        got[d] = swapped(cut(pieces[d]))
    image = imaged(bands[0], pieces[0], got[0], None, token)
    image = imaged(bands[1], pieces[2], got[2], image, image)
    image = imaged(bands[2], pieces[1], pieces[3], image, image)
    projection = leave(bands[3], got[1], got[3], image)
    return volume_next, projection.reshape(angles, 2, depth, detector)


def solution(mesh):
    placed = (
        P("ang", None, "slab", None),
        P("ang", None, None, None),
        P("ang", None),
        P("ang"),
        P(),
        P("ang", None, "slab"),
    )
    return jax.shard_map(
        steps,
        mesh=mesh,
        in_specs=placed,
        out_specs=(P("ang", None, "slab"), P("ang", None, "slab", None)),
        check_vma=False,
    )
```

```python
import functools

import jax
import jax.numpy as jnp
from jax import lax
from jax.experimental import pallas as pl
from jax.experimental.pallas import tpu as pltpu
from jax.sharding import PartitionSpec as P


SMOOTHING = 0.25
YS, ZS, XS, SLABS = 4, 2, 4, 8
LINE = 4
FAR = (2, 1, 3)
ORDER = (*FAR, 0)


def position():
    me, core = lax.axis_index("ang"), lax.axis_index("slab") & 1
    y, zh, x = lax.shift_right_logical(me, 3), lax.shift_right_logical(me, 2) & 1, me & 3
    return y, zh, x, 1 - core


def moved(value, first, delta):
    pairs = []
    for y in range(YS):
        for zh in range(ZS):
            for x in range(XS):
                for slab in range(SLABS):
                    along_x = (slab % 2 == 1) == first
                    ty, tx = (y, (x + delta) % XS) if along_x else ((y + delta) % YS, x)
                    source, target = (y * ZS + zh) * XS + x, (ty * ZS + zh) * XS + tx
                    pairs.append((source * SLABS + slab, target * SLABS + slab))
    return lax.ppermute(value, ("ang", "slab"), pairs)


def across(value):
    return lax.ppermute(value, "ang", [(a, a ^ XS) for a in range(YS * ZS * XS)])


def swapped(value):
    return lax.ppermute(value, "slab", [(i, i ^ 1) for i in range(SLABS)])


def place(d):
    return ORDER.index(d) * LINE


def params(mib, **more):
    return pltpu.CompilerParams(vmem_limit_bytes=mib << 20, **more)


VMEM = pl.BlockSpec(memory_space=pltpu.VMEM)
SMEM = pl.BlockSpec(memory_space=pltpu.SMEM)
ANY = pl.BlockSpec(memory_space=pl.ANY)
AHEAD = pl.CostEstimate(flops=1 << 33, bytes_accessed=1 << 20, transcendentals=0)


def call(kernel, in_specs, outs, flops, mib=16):
    return pl.pallas_call(
        kernel,
        in_specs=in_specs,
        out_specs=[VMEM] * len(outs),
        out_shape=[jax.ShapeDtypeStruct(shape, dtype) for shape, dtype in outs],
        compiler_params=params(mib),
        cost_estimate=pl.CostEstimate(flops=flops, bytes_accessed=1 << 20, transcendentals=0),
    )


def plan_kernel(table):
    y, _, x, own = position()
    for half, owner in enumerate((own, 1 - own)):
        for i, (d, k) in enumerate((d, k) for d in ORDER for k in range(LINE)):
            dy = k + owner * (d - k)
            dx = d + owner * (k - d)
            at = half * len(ORDER) * LINE + i
            table[at] = ((y + dy) & 3) * 8 + owner * 4 + ((x + dx) & 3)


def plan():
    return pl.pallas_call(
        plan_kernel,
        out_specs=SMEM,
        out_shape=jax.ShapeDtypeStruct((2 * len(ORDER) * LINE,), jnp.int32),
        compiler_params=params(4),
        cost_estimate=AHEAD,
        name="plan",
    )()


def edges_kernel(volume, after, cells, inner, outer):
    depth = volume.shape[2]
    core = lax.axis_index("slab") & 1
    for c in range(2):
        turned = volume[:, c, :].T
        cells[c * depth : (c + 1) * depth, :] = turned
        head, tail = turned[:1, :], turned[depth - 1 :, :]
        inner[c : c + 1, :] = jnp.where(core == 0, tail, head)
        outer[c : c + 1, :] = jnp.where(core == 0, head, tail)


def edges(volume, after):
    share, _, depth = volume.shape
    outs = [((2 * depth, share), jnp.float32)] + [((2, share), jnp.float32)] * 2
    return call(edges_kernel, [VMEM, ANY], outs, 1 << 20, 4)(volume, after)


def scale_kernel(table, ids, weights, updates, scaled):
    depth = updates.shape[2]
    for a in range(updates.shape[0]):
        weight = weights[ids[a]]
        for c in range(2):
            at = slice(c * depth, (c + 1) * depth)
            scaled[a, at, :] = (weight * updates[a, c]).astype(jnp.bfloat16)


def scale(updates, table, ids, weights):
    angles, _, depth, detector = updates.shape
    outs = [((angles, 2 * depth, detector), jnp.bfloat16)]
    return call(scale_kernel, [SMEM, SMEM, SMEM, VMEM], outs, 1 << 33, 8)(
        table, ids, weights, updates
    )[0]


def product(sources, tiles, starts, j):
    angles, _, _, block = tiles.shape
    rows = []
    for source in sources:
        windows = []
        for a in range(angles):
            start = pl.multiple_of(starts[a, j] * block, block)
            windows.append(source[a, :, pl.ds(start, 2 * block)])
        rows.append(jnp.concatenate(windows, axis=1))
    weights = jnp.concatenate([tiles[a, j] for a in range(angles)], axis=0)
    return jnp.dot(
        jnp.concatenate(rows, axis=0), weights, preferred_element_type=jnp.float32
    )


def own_kernel(ds, table, starts, scaled, tiles, *outs):
    for d, out in zip(ds, outs):
        for k in range(LINE):
            j = table[place(d) + k]
            out[k] = product((scaled,), tiles, starts, j).astype(out.dtype)


def own_rows(scaled, tiles, table, starts, ds):
    angles, _, band, block = tiles.shape
    rows = scaled.shape[1]
    outs = [((LINE, rows, block), jnp.bfloat16)] * len(ds)
    flops = 2 * len(ds) * LINE * angles * rows * band * block
    kernel = functools.partial(own_kernel, ds)
    return call(kernel, [SMEM, SMEM, VMEM, VMEM], outs, flops)(
        table, starts, scaled, tiles
    )


def join_kernel(d, table, starts, other, tiles, own, after, out):
    rows = other.shape[1]
    for k in range(LINE):
        j = table[place(d) + k]
        out[k, :rows, :] = own[k]
        out[k, rows:, :] = product((other,), tiles, starts, j).astype(out.dtype)


def joined(other, tiles, table, starts, d, own, after):
    angles, _, band, block = tiles.shape
    rows = other.shape[1]
    outs = [((LINE, 2 * rows, block), jnp.bfloat16)]
    flops = 2 * LINE * angles * rows * band * block
    kernel = functools.partial(join_kernel, d)
    specs = [SMEM, SMEM, VMEM, VMEM, VMEM, ANY]
    return call(kernel, specs, outs, flops)(table, starts, other, tiles, own, after)[0]


def both_kernel(d, table, starts, scaled, other, tiles, after, out):
    for k in range(LINE):
        j = table[place(d) + k]
        out[k] = product((scaled, other), tiles, starts, j).astype(out.dtype)


def both_rows(scaled, other, tiles, table, starts, d, dtype, after):
    angles, _, band, block = tiles.shape
    rows = 2 * scaled.shape[1]
    flops = 2 * LINE * angles * rows * band * block
    kernel = functools.partial(both_kernel, d)
    specs = [SMEM, SMEM, VMEM, VMEM, VMEM, ANY]
    return call(kernel, specs, [((LINE, rows, block), dtype)], flops)(
        table, starts, scaled, other, tiles, after
    )[0]


def line_kernel(own, s1, s2, s3, kept, *sent):
    for k in range(LINE):
        total = own[k]
        for ref in (s1, s2, s3):
            total = total + ref[k].astype(jnp.float32)
        if k == 0:
            kept[...] = total
        else:
            sent[k - 1][...] = total.astype(jnp.bfloat16)


def line_sum(own, arrived):
    tile = own.shape[1:]
    outs = [(tile, jnp.float32)] + [(tile, jnp.bfloat16)] * (LINE - 1)
    kept, *sent = call(line_kernel, [VMEM] * 4, outs, 1 << 20)(own, *arrived)
    return kept, sent


def smooth_kernel(cells, inner, outer, smooth):
    rows, share = cells.shape
    depth = rows // 2
    core = lax.axis_index("slab") & 1
    before = jnp.where(core == 0, outer[...], inner[...])
    after = jnp.where(core == 0, inner[...], outer[...])
    z = lax.broadcasted_iota(jnp.int32, (depth, share), 0)
    for c in range(2):
        at = slice(c * depth, (c + 1) * depth)
        value = cells[at, :]
        down = jnp.where(z == 0, before[c : c + 1, :], pltpu.roll(value, 1, 0))
        up = jnp.where(z == depth - 1, after[c : c + 1, :], pltpu.roll(value, depth - 1, 0))
        smooth[at, :] = value - SMOOTHING * (2.0 * value - down - up)


def smoothed(cells, inner, outer):
    outs = [(cells.shape, jnp.float32)]
    return call(smooth_kernel, [VMEM] * 3, outs, 1 << 20, 4)(cells, inner, outer)[0]


def merge_kernel(smooth, beside, own, s1, s2, s3, mine, message):
    _, zh, _, owner = position()
    rows = smooth.shape[0]
    for at, part in ((slice(0, rows), smooth), (slice(rows, 2 * rows), beside)):
        total = own[at, :]
        for ref in (s1, s2, s3):
            total = total + ref[at, :].astype(jnp.float32)
        total = jnp.where(zh == owner, total + part[...], total)
        mine[at, :] = total
        message[at, :] = total.astype(message.dtype)


def merged(smooth, beside, own, reached):
    outs = [(own.shape, jnp.float32), (own.shape, jnp.bfloat16)]
    return call(merge_kernel, [VMEM] * 6, outs, 1 << 20, 4)(
        smooth, beside, own, *reached
    )


def finish_kernel(mine, crossed, own, beside, lowered):
    rows, _ = own.shape
    depth = rows // 2
    for slab, out in enumerate((own, beside)):
        for c in range(2):
            at = slice(slab * rows + c * depth, slab * rows + (c + 1) * depth)
            value = mine[at, :] + crossed[at, :].astype(jnp.float32)
            if c == 1:
                value = jnp.maximum(value, 0.0)
            out[c * depth : (c + 1) * depth, :] = value
            lowered[at, :] = value.astype(lowered.dtype)


def finished(mine, crossed):
    rows, share = mine.shape
    outs = [((rows // 2, share), jnp.float32)] * 2 + [(mine.shape, jnp.bfloat16)]
    return call(finish_kernel, [VMEM] * 2, outs, 1 << 20, 4)(mine, crossed)


def turn_kernel(own, received, volume, token):
    token[...] = jnp.zeros_like(token)
    _, zh, _, owner = position()
    depth = volume.shape[2]
    for c in range(2):
        at = slice(c * depth, (c + 1) * depth)
        volume[:, c, :] = jnp.where(zh == owner, own[at, :], received[at, :]).T


def turned(own, received, shape):
    outs = [(shape, jnp.float32), ((8, 128), jnp.float32)]
    return call(turn_kernel, [VMEM] * 2, outs, 1 << 20, 4)(own, received)


COLUMNS = (((0, 0), (1, 0)), ((0, 2), (1, 2)), ((0, 1), (0, 3)), ((1, 1), (1, 3)))


def spread_kernel(table, starts, tiles, after, *outs):
    block = tiles.shape[3]
    zeros = jnp.zeros((block, block), tiles.dtype)

    def angle(a, carry):
        for out, groups in zip(outs, COLUMNS):
            for i in range(2 * LINE):
                half, d = groups[i // LINE]
                j = table[half * len(ORDER) * LINE + place(d) + i % LINE]
                first = starts[a, j]
                column = slice(i * block, (i + 1) * block)
                for empty in (jnp.where(first == 0, 2, 0), jnp.where(first == 2, 1, 3)):
                    at = pl.ds(pl.multiple_of(empty * block, block), block)
                    out[a, at, column] = zeros
                at = pl.ds(pl.multiple_of(first * block, block), 2 * block)
                out[a, at, column] = tiles[a, j]
        return carry

    lax.fori_loop(0, tiles.shape[0], angle, 0)


def spread(tiles, table, starts, detector, after):
    angles, _, _, block = tiles.shape
    outs = [((angles, detector, 2 * LINE * block), tiles.dtype)] * len(COLUMNS)
    return call(spread_kernel, [SMEM, SMEM, VMEM, ANY], outs, 1 << 31, 16)(
        table, starts, tiles, after
    )


def cut_kernel(*refs):
    *parts, out = refs
    at = 0
    for part in parts:
        count = part.shape[0]
        out[at : at + count] = part[:, out.shape[1] :, :]
        at += count


def cut(parts):
    _, rows, block = parts[0].shape
    outs = [((LINE, rows // 2, block), parts[0].dtype)]
    return call(cut_kernel, [VMEM] * len(parts), outs, 1 << 18, 4)(*parts)[0]


def projected(blocks, weights):
    row = jnp.concatenate(blocks, axis=1)
    return lax.dot_general(
        row, weights, (((1,), (1,)), ((), ())), preferred_element_type=jnp.float32
    )


def image_kernel(chained, weights, *refs):
    *refs, after, image = refs
    *parts, before = refs if chained else (*refs, None)
    rows = image.shape[1]
    blocks = [part[k, :rows, :] for part in parts for k in range(part.shape[0])]
    for a in range(image.shape[0]):
        value = projected(blocks, weights[a])
        image[a] = before[a] + value if chained else value


def imaged(weights, parts, before, after):
    angles, detector, _ = weights.shape
    rows = parts[0].shape[1] // 2
    more = [] if before is None else [before]
    outs = [((angles, rows, detector), jnp.float32)]
    kernel = functools.partial(image_kernel, before is not None)
    specs = [VMEM] * (1 + len(parts) + len(more)) + [ANY]
    return call(kernel, specs, outs, 2 * weights.size * rows)(weights, *parts, *more, after)[0]


def leave_kernel(weights, one, two, before, out, image, done):
    blocks = [piece[k] for piece in (one, two) for k in range(LINE)]
    copies = []
    for a in range(image.shape[0]):
        image[a] = before[a] + projected(blocks, weights[a])
        copies.append(pltpu.make_async_copy(image.at[a], out.at[a], done.at[a]))
        copies[-1].start()
    for copy in copies:
        copy.wait()


def leave(weights, one, two, before):
    shape = before.shape
    return pl.pallas_call(
        leave_kernel,
        in_specs=[VMEM] * 4,
        out_specs=ANY,
        out_shape=jax.ShapeDtypeStruct(shape, jnp.float32),
        scratch_shapes=[pltpu.VMEM(shape, jnp.float32), pltpu.SemaphoreType.DMA((shape[0],))],
        compiler_params=params(16),
        cost_estimate=pl.CostEstimate(flops=1 << 29, bytes_accessed=1 << 20, transcendentals=0),
        name="leave",
    )(weights, one, two, before)


def steps(updates, tiles, starts, ids, weights, volume):
    angles, _, depth, detector = updates.shape
    count = lax.axis_size("slab")
    table = plan()
    scaled = scale(updates, table, ids, weights)
    other = swapped(scaled)
    own2, own1 = own_rows(scaled, tiles, table, starts, (2, 1))
    sent = {}
    sent[2] = joined(other, tiles, table, starts, 2, own2, own1)
    sent[1] = joined(other, tiles, table, starts, 1, own1, sent[2])
    sent[3] = both_rows(scaled, other, tiles, table, starts, 3, jnp.bfloat16, sent[1])
    own = both_rows(scaled, other, tiles, table, starts, 0, jnp.float32, sent[3])
    arrived = []
    for d in FAR:
        arrived.append(moved(sent[d], True, d))

    cells, inner, outer = edges(volume, own)
    inner = swapped(inner)
    odd = range(1, count - 1, 2)
    outer = lax.ppermute(outer, "slab", [p for i in odd for p in ((i, i + 1), (i + 1, i))])
    smooth = smoothed(cells, inner, outer)
    beside = swapped(smooth)
    kept, passed = line_sum(own, arrived)
    reached = []
    for d in FAR:
        reached.append(moved(passed[d - 1], False, d))
    mine, message = merged(smooth, beside, kept, reached)
    crossed = across(message)
    bands = spread(tiles, table, starts, detector, message)
    own, beside, lowered = finished(mine, crossed)

    came = {}
    for d in FAR:
        came[d] = moved(lowered, False, LINE - d)
    early = {}
    for d in FAR[1:]:
        early[d] = moved(lowered, True, LINE - d)
    beside, came[1], came[2], came[3] = lax.optimization_barrier(
        (beside, came[1], came[2], came[3])
    )
    short = [came[d] for d in range(1, LINE)]
    line, rest = jnp.stack([lowered, *short]), jnp.stack(short)
    pieces = {0: [line]}
    for d in FAR:
        came = moved(rest if d in early else line, True, LINE - d)
        pieces[d] = [early[d][None], came] if d in early else [came]
    received = swapped(beside)
    volume_next, token = turned(own, received, volume.shape)
    got = {}
    for d in (0, *FAR):
        got[d] = swapped(cut(pieces[d]))
    image = imaged(bands[0], [*pieces[0], got[0]], None, token)
    image = imaged(bands[1], [*pieces[2], got[2]], image, image)
    image = imaged(bands[2], [*pieces[1], *pieces[3]], image, image)
    projection = leave(bands[3], got[1], got[3], image)
    return volume_next, projection.reshape(angles, 2, depth, detector)


def solution(mesh):
    placed = (
        P("ang", None, "slab", None),
        P("ang", None, None, None),
        P("ang", None),
        P("ang"),
        P(),
        P("ang", None, "slab"),
    )
    return jax.shard_map(
        steps,
        mesh=mesh,
        in_specs=placed,
        out_specs=(P("ang", None, "slab"), P("ang", None, "slab", None)),
        check_vma=False,
    )
```
